32 devices in a mesh: dp: 16 (over z, x, core), head: 2 (over y).
Axes of the slice: x: 2, y: 2, z: 4, core: 2. Of those that a mesh axis runs over, the one named last changes fastest.
Arguments:
- frames_in: bfloat16 [16, 2, 320, 2560], P('dp', 'head'), may hold values from -6 to 6
- ln1_gain: float32 [1280], replicated, may hold values from 0.25 to 1.75
- ln1_bias: float32 [1280], replicated, may hold values from -3 to 3
- qkv_weight: bfloat16 [1280, 3, 1024], P('dp', None, 'head'), may hold values from -0.1875 to 0.1875
- qv_bias: float32 [2, 1024], P(None, 'head'), may hold values from -3 to 3
- out_weight: bfloat16 [1024, 1280], P(('head', 'dp')), may hold values from -0.1875 to 0.1875
- out_bias: float32 [1280], P('head'), may hold values from -3 to 3
- ln2_gain: float32 [1280], replicated, may hold values from 0.25 to 1.75
- ln2_bias: float32 [1280], replicated, may hold values from -3 to 3
- fc1_weight: bfloat16 [1280, 5120], P('dp', 'head'), may hold values from -0.15625 to 0.15625
- fc1_bias: float32 [5120], P('head'), may hold values from -3 to 3
- fc2_weight: bfloat16 [5120, 1280], P(('head', 'dp')), may hold values from -0.078125 to 0.078125
- fc2_bias: float32 [1280], P('head'), may hold values from -3 to 3
- server_of_clip: int32 [16], replicated, may hold values from 0 to 7
Outputs:
- encoded: bfloat16 [16, 2, 320, 2560], P('dp', 'head')
The draws below stay inside these ranges and needn't reach their ends.
All inputs are finite; a program needn't handle non-finite values.
Results may differ from the reference program's by a relative error of at most 0.014.
Values may be sent and summed in bfloat16 or wider, within the bound.
A program may use at most 64 MiB of HBM per device.

```python
import jax
import jax.numpy as jnp
from jax import lax

D = 1280
HEADS = 16
HDIM = 64
MLP = 5120
FRAMES = 1280
SERVERS = 8
CLIPS = 16
N_HEAD = 2


def draw_qkv_weight(key, part):
    normal = jax.random.normal(jax.random.fold_in(key, 29), (D, 3, HEADS * HDIM), jnp.float32)
    return jnp.clip(normal * D ** (-0.5), -0.1875, 0.1875).astype(jnp.bfloat16)


def plant(entries, own_key, low, high):
    index_at = [jax.random.randint(jax.random.fold_in(own_key, axis), (), 0, length) for axis, length in enumerate(entries.shape)]
    widest = entries.shape.index(max(entries.shape))
    next_to = index_at[:widest] + [(index_at[widest] + 1) % entries.shape[widest]] + index_at[widest + 1:]
    return entries.at[tuple(index_at)].set(low).at[tuple(next_to)].set(high)


def block_levels(own_key, extent, split, low, top_value):
    level, own = 1.0, jax.random.fold_in(own_key, 6)
    for axis_at, shards_of in split:
        heights = jnp.exp(jax.random.uniform(jax.random.fold_in(own, axis_at), (shards_of,), jnp.float32, low / len(split), top_value / len(split)))
        level = level * jnp.repeat(heights, extent[axis_at] // shards_of).reshape([-1 if axis == axis_at else 1 for axis in range(len(extent))])
    return level


def noise(own_key, extent, deviation, most, split=(), held_as=jnp.bfloat16):
    level = block_levels(own_key, extent, split, -0.22, 0.18) if split else 1.0
    values = jax.random.normal(own_key, extent, jnp.float32) * deviation * level
    return jnp.minimum(jnp.maximum(values, -most), most).astype(held_as)


def setup_inputs(seed: int = 0) -> dict:
    streams_of = jax.random.split(jax.random.key(seed), 15)
    return {
        "frames_in": noise(streams_of[0], (CLIPS, N_HEAD, FRAMES // 4, 4 * D // N_HEAD), 1.0, 6.0, ((0, 16), (1, 2))),
        "ln1_gain": jnp.clip(1.0 + 0.15 * jax.random.normal(streams_of[1], (D,), jnp.float32), 0.25, 1.75),
        "ln1_bias": noise(streams_of[2], (D,), 0.5, 3.0, (), jnp.float32),
        "qkv_weight": draw_qkv_weight(jax.random.fold_in(streams_of[14], 71), 0),
        "qv_bias": noise(streams_of[4], (2, HEADS * HDIM), 0.5, 3.0, ((1, 2),), jnp.float32),
        "out_weight": noise(streams_of[5], (HEADS * HDIM, D), (HEADS * HDIM) ** -0.5, 0.1875, ((0, 32),)),
        "out_bias": noise(streams_of[6], (D,), 0.5, 3.0, ((0, 2),), jnp.float32),
        "ln2_gain": jnp.clip(1.0 + 0.15 * jax.random.normal(streams_of[7], (D,), jnp.float32), 0.25, 1.75),
        "ln2_bias": noise(streams_of[8], (D,), 0.5, 3.0, (), jnp.float32),
        "fc1_weight": noise(streams_of[9], (D, MLP), D ** -0.5, 0.15625, ((0, 16), (1, 2))),
        "fc1_bias": noise(streams_of[10], (MLP,), 0.5, 3.0, ((0, 2),), jnp.float32),
        "fc2_weight": noise(streams_of[11], (MLP, D), MLP ** -0.5, 0.078125, ((0, 32),)),
        "fc2_bias": noise(streams_of[12], (D,), 0.5, 3.0, ((0, 2),), jnp.float32),
        "server_of_clip": plant(jax.random.randint(streams_of[13], (CLIPS,), 0, SERVERS), jax.random.fold_in(streams_of[13], 1), 0, SERVERS - 1).astype(jnp.int32),
    }


epsilon = 1e-05

def layer_norm(matrix, gain_row, shift_row):
    floats = matrix.astype(jnp.float32)
    center = lax.optimization_barrier(jnp.mean(floats, axis=-1, keepdims=True))
    spread = lax.optimization_barrier(jnp.mean(jnp.square(floats - center), axis=-1, keepdims=True))
    return ((floats - center) * lax.rsqrt(spread + epsilon) * gain_row + shift_row).astype(jnp.bfloat16)

def attend(queries, key_rows, value_rows):

    def single(triple):
        query_head, key_head, value_head = triple
        scores = jnp.dot(query_head, key_head.T, preferred_element_type=jnp.float32)
        maxima = lax.optimization_barrier(jnp.max(scores, axis=-1, keepdims=True))
        weights = jnp.exp(scores - maxima)
        probability = (weights / lax.optimization_barrier(jnp.sum(weights, axis=-1, keepdims=True))).astype(jnp.bfloat16)
        return jnp.dot(probability, value_head, preferred_element_type=jnp.float32).astype(jnp.bfloat16)
    per_head = lax.map(single, (jnp.swapaxes(queries, 0, 1), jnp.swapaxes(key_rows, 0, 1), jnp.swapaxes(value_rows, 0, 1)))
    return jnp.swapaxes(per_head, 0, 1).reshape(queries.shape[0], -1)

def slot_order(server_list):
    clip_count = server_list.shape[0]
    indices = jnp.arange(clip_count, dtype=jnp.int32)
    earlier = (server_list[None, :] < server_list[:, None]) | (server_list[None, :] == server_list[:, None]) & (indices[None, :] < indices[:, None])
    slot_of = lax.optimization_barrier(jnp.sum(earlier.astype(jnp.int32), axis=1)).astype(jnp.int32)
    return lax.optimization_barrier(jnp.sum(jnp.where(slot_of[None, :] == indices[:, None], indices[None, :], 0), axis=1)).astype(jnp.int32)

def reference(frames_in, ln1_gain, ln1_bias, qkv_weight, qv_bias, out_weight, out_bias, ln2_gain, ln2_bias, fc1_weight, fc1_bias, fc2_weight, fc2_bias, server_of_clip):
    block_width = D // N_HEAD
    clip_total = frames_in.shape[0]
    residual_all = frames_in.reshape(clip_total, N_HEAD, FRAMES // 4, 4, block_width).transpose(0, 2, 3, 1, 4).reshape(clip_total, FRAMES, D)

    def clip_layer(residual_in):
        frame_count = residual_in.shape[0]
        normed_one = layer_norm(residual_in, ln1_gain, ln1_bias)
        column_count = qkv_weight.shape[2]
        projected = jnp.dot(normed_one, qkv_weight.reshape(qkv_weight.shape[0], 3 * column_count), preferred_element_type=jnp.float32).reshape(frame_count, 3, column_count)
        queries = ((projected[:, 0] + qv_bias[0]) * HDIM ** (-0.5)).astype(jnp.bfloat16).reshape(frame_count, -1, HDIM)
        key_rows = projected[:, 1].astype(jnp.bfloat16).reshape(frame_count, -1, HDIM)
        value_rows = (projected[:, 2] + qv_bias[1]).astype(jnp.bfloat16).reshape(frame_count, -1, HDIM)
        context = attend(queries, key_rows, value_rows)
        attended = (residual_in.astype(jnp.float32) + out_bias + jnp.dot(context, out_weight, preferred_element_type=jnp.float32)).astype(jnp.bfloat16)
        normed_two = layer_norm(attended, ln2_gain, ln2_bias)
        hidden = jax.nn.gelu(jnp.dot(normed_two, fc1_weight, preferred_element_type=jnp.float32) + fc1_bias, approximate=False).astype(jnp.bfloat16)
        return (attended.astype(jnp.float32) + fc2_bias + jnp.dot(hidden, fc2_weight, preferred_element_type=jnp.float32)).astype(jnp.bfloat16)
    layer_out = lax.map(clip_layer, residual_all)
    clip_order = slot_order(server_of_clip)
    ordered = jnp.take(layer_out, clip_order, axis=0)
    return ordered.reshape(clip_total, FRAMES // 4, 4, N_HEAD, block_width).transpose(0, 3, 1, 2, 4).reshape(clip_total, N_HEAD, FRAMES // 4, 4 * block_width)
```

```python
import functools

import jax
import jax.numpy as jnp
from jax import lax
from jax.experimental import pallas as pl
from jax.experimental.pallas import tpu as pltpu
from jax.sharding import PartitionSpec as P

HDIM = 64


epsilon = 1e-05


def layer_norm(matrix, gain_row, shift_row):
    floats = matrix.astype(jnp.float32)
    center = jnp.mean(floats, axis=-1, keepdims=True)
    spread = jnp.mean(jnp.square(floats - center), axis=-1, keepdims=True)
    return ((floats - center) * lax.rsqrt(spread + epsilon) * gain_row + shift_row).astype(
        jnp.bfloat16
    )


def normalize(residual_in, gain_row, shift_row):
    whole_rows = lax.all_gather(residual_in, "head", axis=1, tiled=True)
    return layer_norm(whole_rows, gain_row, shift_row)


def attend(queries, key_rows, value_rows):

    def single(triple):
        query_head, key_head, value_head = triple
        scores = jnp.dot(query_head, key_head.T, preferred_element_type=jnp.float32)
        maxima = jnp.max(scores, axis=-1, keepdims=True)
        weights = jnp.exp(scores - maxima)
        probability = (weights / jnp.sum(weights, axis=-1, keepdims=True)).astype(jnp.bfloat16)
        return jnp.dot(probability, value_head, preferred_element_type=jnp.float32).astype(
            jnp.bfloat16
        )

    per_head = lax.map(
        single,
        (jnp.swapaxes(queries, 0, 1), jnp.swapaxes(key_rows, 0, 1), jnp.swapaxes(value_rows, 0, 1)),
    )
    return jnp.swapaxes(per_head, 0, 1).reshape(queries.shape[0], -1)


def slot_order(server_list):
    clip_count = server_list.shape[0]
    indices = jnp.arange(clip_count, dtype=jnp.int32)
    earlier = (server_list[None, :] < server_list[:, None]) | (
        server_list[None, :] == server_list[:, None]
    ) & (indices[None, :] < indices[:, None])
    slot_of = jnp.sum(earlier.astype(jnp.int32), axis=1)
    return jnp.sum(jnp.where(slot_of[None, :] == indices[:, None], indices[None, :], 0), axis=1)


def regroup(block_rows, clip_order):
    group_size = lax.axis_size("dp")
    piece_rows = block_rows.reshape(group_size, -1)
    shuffled = lax.all_to_all(piece_rows, "dp", split_axis=0, concat_axis=0, tiled=True)
    picked = jnp.take(shuffled, clip_order, axis=0)
    returned = lax.all_to_all(picked, "dp", split_axis=0, concat_axis=0, tiled=True)
    return returned.reshape(block_rows.shape)


def block_term(operand, weight_rows, row_count, frame_count, local_width):
    blocks = row_count // frame_count
    product = jnp.dot(operand, weight_rows, preferred_element_type=jnp.float32)
    return (
        product.reshape(frame_count, blocks, local_width)
        .transpose(1, 0, 2)
        .reshape(blocks * frame_count, local_width)
    )


def on_device(
    frames_in,
    ln1_gain,
    ln1_bias,
    qkv_weight,
    qv_bias,
    out_weight,
    out_bias,
    ln2_gain,
    ln2_bias,
    fc1_weight,
    fc1_bias,
    fc2_weight,
    fc2_bias,
    server_of_clip,
):
    clip_order = slot_order(server_of_clip)
    group_rows = frames_in.shape[2]
    local_width = frames_in.shape[3] // 4
    frame_count = group_rows * 4
    residual_in = frames_in[0, 0].reshape(frame_count, local_width)
    residual_in = regroup(residual_in, clip_order)
    normed_one = normalize(residual_in, ln1_gain, ln1_bias)
    column_count = qkv_weight.shape[2]
    weight_piece = lax.all_gather(qkv_weight, "dp", axis=0, tiled=True)
    operand = normed_one
    projected = jnp.dot(
        operand, weight_piece.reshape(weight_piece.shape[0], -1), preferred_element_type=jnp.float32
    ).reshape(frame_count, 3, column_count)
    queries = (
        ((projected[:, 0] + qv_bias[0]) * HDIM ** (-0.5))
        .astype(jnp.bfloat16)
        .reshape(frame_count, -1, HDIM)
    )
    key_rows = projected[:, 1].astype(jnp.bfloat16).reshape(frame_count, -1, HDIM)
    value_rows = (projected[:, 2] + qv_bias[1]).astype(jnp.bfloat16).reshape(frame_count, -1, HDIM)
    context = attend(queries, key_rows, value_rows)
    output_rows = lax.all_gather(out_weight, "dp", axis=0, tiled=True)
    carried = residual_in.astype(jnp.float32) + out_bias
    attended = (
        carried
        + lax.psum_scatter(
            block_term(
                context, output_rows, frame_count * lax.axis_size("head"), frame_count, local_width
            ).astype(jnp.bfloat16),
            "head",
            scatter_dimension=0,
            tiled=True,
        ).astype(jnp.float32)
    ).astype(jnp.bfloat16)
    normed_two = normalize(attended, ln2_gain, ln2_bias)
    operand = normed_two
    hidden_sums = jnp.dot(
        operand,
        lax.all_gather(fc1_weight, "dp", axis=0, tiled=True),
        preferred_element_type=jnp.float32,
    )
    hidden = jax.nn.gelu(hidden_sums + fc1_bias, approximate=False).astype(jnp.bfloat16)
    down_rows = lax.all_gather(fc2_weight, "dp", axis=0, tiled=True)
    kept = attended.astype(jnp.float32) + fc2_bias
    layer_out = (
        kept
        + lax.psum_scatter(
            block_term(
                hidden, down_rows, frame_count * lax.axis_size("head"), frame_count, local_width
            ).astype(jnp.bfloat16),
            "head",
            scatter_dimension=0,
            tiled=True,
        ).astype(jnp.float32)
    ).astype(jnp.bfloat16)
    return layer_out.reshape(1, 1, group_rows, 4 * local_width)


MESH = pl.DeviceIdType.MESH
VMEM = pltpu.MemorySpace.VMEM
ANY = pl.ANY
CORES = 2
PAIR = 2 * HDIM
UP, DOWN, SIDE, CORE = range(4)


def at_rows(index, rows):
    return pl.ds(pl.multiple_of(index * rows, rows), rows)


def norm_rows(floats, gain, shift):
    center = jnp.mean(floats, axis=-1, keepdims=True)
    moved = floats - center
    spread = jnp.mean(jnp.square(moved), axis=-1, keepdims=True)
    return (moved * lax.rsqrt(spread + epsilon) * gain + shift).astype(jnp.bfloat16)


def loop(start, stop, body):
    def step(k, carry):
        body(k)
        return carry

    lax.fori_loop(start, stop, step, 0)


class Gather:
    def __init__(self, me, h, dp, parts, send, recv):
        self.h, self.parts, self.send, self.recv = h, parts, send, recv
        self.sides = 2
        self.length = dp // (self.sides * CORES)
        self.core = lax.rem(me, CORES)
        self.side = lax.rem(lax.div(me, CORES), self.sides)
        self.z = lax.div(me, CORES * self.sides)
        self.started = []

    def index(self, z, side, core):
        return (z * self.sides + side) * CORES + core

    def copy(self, t, origin, route):
        target = {
            UP: lambda: self.index(self.z + 1, self.side, self.core),
            DOWN: lambda: self.index(self.z - 1, self.side, self.core),
            SIDE: lambda: self.index(self.z, 1 - self.side, self.core),
            CORE: lambda: self.index(self.z, self.side, 1 - self.core),
        }[route]()
        ref = self.parts[t](origin)
        return pltpu.make_async_remote_copy(
            ref, ref, self.send.at[t, route, origin], self.recv.at[t, origin], (target, self.h), MESH
        )

    def go(self, t, origin, routes, act):
        for route in routes:
            copy = self.copy(t, origin, route)
            if route == UP:
                pl.when(self.z < self.length - 1)(lambda copy=copy: act(copy))
            elif route == DOWN:
                pl.when(self.z > 0)(lambda copy=copy: act(copy))
            else:
                act(copy)

    def own(self, t, act):
        self.go(t, self.index(self.z, self.side, self.core), (UP, DOWN, SIDE, CORE), act)

    def line(self, t, s, act, arrive=True):
        @pl.when(self.z >= s)
        def _():
            origin = self.index(self.z - s, self.side, self.core)
            if arrive:
                self.copy(t, origin, CORE).wait_recv()
            self.go(t, origin, (UP, SIDE, CORE), act)

        @pl.when(self.z + s < self.length)
        def _():
            origin = self.index(self.z + s, self.side, self.core)
            if arrive:
                self.copy(t, origin, CORE).wait_recv()
            self.go(t, origin, (DOWN, SIDE, CORE), act)

    def across(self, t, s, act, arrive=True):
        def one(z):
            origin = self.index(z, 1 - self.side, self.core)
            if arrive:
                self.copy(t, origin, CORE).wait_recv()
            self.go(t, origin, (CORE,), act)

        if s == 0:
            one(self.z)
            return
        pl.when(self.z >= s)(lambda: one(self.z - s))
        pl.when(self.z + s < self.length)(lambda: one(self.z + s))

    def rest(self, t):
        def one(k):
            origin = k * CORES + 1 - self.core
            self.copy(t, origin, CORE).wait_recv()

        loop(0, self.length * self.sides, one)

    def finish(self, t):
        act = lambda copy: copy.wait_send()
        self.own(t, act)
        for s in range(1, self.length):
            self.line(t, s, act, False)
        for s in range(self.length):
            self.across(t, s, act, False)


def layer_kernel(
    dp,
    sizes,
    order_ref,
    par_ref,
    x_ref,
    wq_ref,
    wo_ref,
    w1_ref,
    w2_ref,
    o_ref,
    all_q,
    all_o,
    all_1,
    all_2,
    x,
    q,
    k,
    v,
    ctx,
    att,
    second,
    full,
    normed,
    hidden,
    out,
    got,
    kept,
    done,
    wsend,
    wrecv,
    own_sem,
    xs,
    xr,
    xo,
    os_,
    or_,
    cs,
    cr,
    s1,
    r1,
    s2,
    r2,
    s3,
    r3,
    fs,
    fr,
    ds,
    *first,
):
    start = lambda copy: copy.start()
    me, h = lax.axis_index("dp"), lax.axis_index("head")
    there = 1 - h
    peer = (me, there)
    groups = x_ref.shape[0]
    width = x_ref.shape[1] // 4
    frames, depth = x.shape
    columns = q.shape[1]
    pairs = columns // PAIR
    blocks, _, rows, _ = second.shape
    block = frames // blocks
    tile = sizes["tile"]
    chunk = sizes["chunk"]
    (g1, b1), (g2, b2), qb, vb, ob, fb, f1 = sizes["offsets"]

    def par(offset, size):
        return par_ref[0:1, offset : offset + size]

    barrier = pltpu.get_barrier_semaphore()

    def hello(n):
        pl.semaphore_signal(barrier, inc=1, device_id=(lax.rem(me + n, dp), h), device_id_type=MESH)

    loop(1, dp, hello)
    pl.semaphore_signal(barrier, inc=1, device_id=peer, device_id_type=MESH)

    parts = [
        lambda d: all_q.at[:, at_rows(d, wq_ref.shape[1]), :],
        lambda d: all_o.at[:, at_rows(d, wo_ref.shape[0]), :],
        lambda d: all_1.at[at_rows(d, w1_ref.shape[0]), :],
        lambda d: all_2.at[at_rows(d, w2_ref.shape[0]), :],
    ]
    net = Gather(me, h, dp, parts, wsend, wrecv)
    mine = [
        pltpu.make_async_copy(wq_ref, parts[0](me), own_sem.at[0]),
        pltpu.make_async_copy(
            wo_ref.at[:, at_rows(h, width)],
            all_o.at[h, at_rows(me, wo_ref.shape[0]), :],
            own_sem.at[1],
        ),
        pltpu.make_async_copy(w1_ref, parts[2](me), own_sem.at[2]),
        pltpu.make_async_copy(w2_ref, parts[3](me), own_sem.at[3]),
    ]
    for copy in mine:
        copy.start()

    def x_part(j):
        return x_ref.at[:, j * width : (j + 1) * width], x.at[
            j * groups : (j + 1) * groups, at_rows(h, width)
        ]

    for j in range(4):
        pltpu.make_async_copy(*x_part(j), xo.at[j]).start()
    mine[0].wait()
    pl.semaphore_wait(barrier, dp)

    half = pltpu.make_async_remote_copy(
        wo_ref.at[:, at_rows(there, width)],
        all_o.at[h, at_rows(me, wo_ref.shape[0]), :],
        os_,
        or_,
        peer,
        MESH,
    )
    half.start()
    net.own(0, start)

    def x_copy(j):
        source, target = x_part(j)
        return pltpu.make_async_remote_copy(source, target, xs.at[j], xr.at[j], peer, MESH)

    for j in range(4):
        x_copy(j).start()

    def out_own():
        mine[1].wait()
        half.wait_recv()
        net.own(1, start)

    def up_own():
        mine[2].wait()
        net.own(2, start)

    def down_own():
        mine[3].wait()
        net.own(3, start)

    L = lambda t, s: lambda: net.line(t, s, start)
    A = lambda t, s: lambda: net.across(t, s, start)
    for step in sizes["early"](L, A, out_own, up_own, down_own):
        step()
    later = sizes["later"](L, A, out_own, up_own, down_own)
    net.rest(0)

    def project(j):
        at = at_rows(j, groups)
        n = norm_rows(x[at, :].astype(jnp.float32), par(g1, depth), par(b1, depth))

        def part(i):
            return jnp.dot(n, all_q[i], preferred_element_type=jnp.float32)

        q[at, :] = ((part(0) + par(qb, columns)) * HDIM ** (-0.5)).astype(jnp.bfloat16)
        k[at, :] = part(1).astype(jnp.bfloat16)
        v[at, :] = (part(2) + par(vb, columns)).astype(jnp.bfloat16)

    for j in range(4):
        pltpu.make_async_copy(*x_part(j), xo.at[j]).wait()
        x_copy(j).wait_recv()

    loop(0, 4, project)

    lane = lax.broadcasted_iota(jnp.int32, (1, PAIR), 1)
    low_f = jnp.where(lane < HDIM, 1.0, 0.0)
    low, high = low_f.astype(jnp.bfloat16), (1.0 - low_f).astype(jnp.bfloat16)

    def attend(b, p):
        cols = at_rows(p, PAIR)
        keys, values = k[:, cols], v[:, cols]

        def head(query, value):
            scores = lax.dot_general(
                query, keys, (((1,), (1,)), ((), ())), preferred_element_type=jnp.float32
            )
            top = jnp.max(scores, axis=-1, keepdims=True)
            weights = jnp.exp(scores - top).astype(jnp.bfloat16)
            return jnp.dot(weights, value, preferred_element_type=jnp.float32)

        at = at_rows(b, block)
        query = q[at, cols]
        one = head(query * low, values * low + high)
        two = head(query * high, values * high + low)
        top = one * low_f + two * (1.0 - low_f)
        total = pltpu.roll(one * (1.0 - low_f) + two * low_f, HDIM, 1)
        ctx[at, at_rows(h * pairs + p, PAIR)] = (top / total).astype(jnp.bfloat16)

    def ctx_copy(b):
        ref = ctx.at[at_rows(b, block), at_rows(h, columns)]
        return pltpu.make_async_remote_copy(ref, ref, cs.at[b], cr.at[b], peer, MESH)

    def attended(b):
        ctx_copy(b).wait_recv()
        at = at_rows(b, block)
        total = x[at, at_rows(h, width)].astype(jnp.float32) + par(ob, width)
        for i in range(2):
            total = total + jnp.dot(
                ctx[at, i * columns : (i + 1) * columns],
                all_o[i],
                preferred_element_type=jnp.float32,
            )
        att[at, :] = total.astype(jnp.bfloat16)

    def piece(ref, b, j):
        return ref.at[at_rows(b * dp + j, rows)]

    def home(b, j):
        return full.at[at_rows(b * dp + j, rows), at_rows(h, width)]

    def one(b, n):
        other = lax.rem(me + n, dp)
        return pltpu.make_async_remote_copy(
            piece(att, b, other), first[b].at[me], s1.at[b, n], r1.at[b, n], (other, h), MESH
        )

    def one_own(b):
        return pltpu.make_async_copy(piece(att, b, me), first[b].at[me], r1.at[b, 0])

    def two(b, n):
        other = lax.rem(me + n, dp)
        return pltpu.make_async_remote_copy(
            second.at[b, other], home(b, me), s2.at[b, n], r2.at[b, n], (other, h), MESH
        )

    def two_own(b):
        return pltpu.make_async_copy(second.at[b, me], home(b, me), r2.at[b, 0])

    def three(b):
        ref = full.at[at_rows(b, block), at_rows(h, width)]
        return pltpu.make_async_remote_copy(ref, ref, s3.at[b], r3.at[b], peer, MESH)

    def spread(b):
        one_own(b).start()
        loop(1, dp, lambda n: one(b, n).start())

    def pick(b):
        one_own(b).wait()
        loop(1, dp, lambda n: one(b, n).wait_recv())

        def choose(s):
            second[b, s] = first[b][order_ref[s]]

        loop(0, dp, choose)
        two_own(b).start()
        loop(1, dp, lambda n: two(b, n).start())

    def forward(b):
        two_own(b).wait()
        loop(1, dp, lambda n: two(b, n).wait_recv())
        three(b).start()

    def share(target):
        return jnp.dot(
            hidden[...], all_2[:, at_rows(target, width)], preferred_element_type=jnp.float32
        )

    def out_copy(b):
        return pltpu.make_async_remote_copy(
            out.at[b], got.at[b], fs.at[b], fr.at[b], peer, MESH
        )

    def feed(b):
        three(b).wait_recv()
        at = at_rows(b, block)
        normed[...] = norm_rows(full[at, :].astype(jnp.float32), par(g2, depth), par(b2, depth))

        for t in range(hidden.shape[1] // tile):
            cols = slice(t * tile, (t + 1) * tile)
            sums = jnp.dot(normed[...], all_1[:, cols], preferred_element_type=jnp.float32)
            sums = sums + par(f1 + t * tile, tile)
            hidden[:, cols] = (0.5 * sums * (1.0 + lax.erf(sums * 0.7071067811865476))).astype(
                jnp.bfloat16
            )

        out[b] = share(there).astype(jnp.bfloat16)
        out_copy(b).start()
        kept[b] = full[at, at_rows(h, width)].astype(jnp.float32) + par(fb, width) + share(h)

    def done_copy(b, i):
        n = b * (block // chunk) + i
        per = groups // chunk
        return pltpu.make_async_copy(
            done.at[at_rows(n, chunk)],
            o_ref.at[at_rows(lax.rem(n, per), chunk), at_rows(lax.div(n, per), width)],
            ds.at[b, i],
        )

    def close(b):
        out_copy(b).wait_recv()
        done[at_rows(b, block), :] = (kept[b] + got[b].astype(jnp.float32)).astype(jnp.bfloat16)
        loop(0, block // chunk, lambda i: done_copy(b, i).start())

    def when(i, offset, body):
        b = i - offset

        @pl.when((b >= 0) & (b < blocks))
        def _():
            body(b)

    def each_static(b, body):
        for n in range(blocks):
            pl.when(b == n)(lambda n=n: body(n))

    o_out, o_pick, o_forward, o_feed, o_close = sizes["stages"]

    def master(i):
        def attend_block(b):
            def each(p):
                attend(b, p)
                for n, step in enumerate(later):
                    pl.when(b * pairs + p == n)(step)

            loop(0, pairs, each)
            ctx_copy(b).start()

        when(i, 0, attend_block)

        def out_block(b):
            pl.when(b == 0)(lambda: net.rest(1))
            attended(b)
            each_static(b, spread)

        when(i, o_out, out_block)
        when(i, o_pick, lambda b: each_static(b, pick))
        when(i, o_forward, forward)

        def feed_block(b):
            @pl.when(b == 0)
            def _():
                for step in later[blocks * pairs :]:
                    step()
                net.rest(2)
                net.rest(3)

            feed(b)

        when(i, o_feed, feed_block)
        when(i, o_close, close)

    loop(0, blocks + o_close, master)

    for t in range(4):
        net.finish(t)
    half.wait_send()
    for j in range(4):
        x_copy(j).wait_send()

    def last(b):
        ctx_copy(b).wait_send()
        three(b).wait_send()
        out_copy(b).wait_send()
        loop(1, dp, lambda n: two(b, n).wait_send())
        loop(0, block // chunk, lambda i: done_copy(b, i).wait())

    loop(0, blocks, last)
    for b in range(blocks):
        loop(1, dp, lambda n: one(b, n).wait_send())


def early(L, A, out_own, up_own, down_own):
    return [
        out_own, L(0, 1), up_own, L(1, 1), L(0, 2), A(0, 0), A(1, 0), L(1, 2), L(0, 3), A(0, 1),
        A(1, 1), L(1, 3), A(0, 2), L(2, 1), A(1, 2), down_own, A(0, 3), A(1, 3),
    ]


def later(L, A, out_own, up_own, down_own):
    return [
        A(2, 0), L(2, 2), L(2, 3), A(2, 1), L(3, 1), A(3, 0), A(2, 2), L(3, 2), A(2, 3), L(3, 3),
        A(3, 1), A(3, 2), A(3, 3),
    ]


def on_device_aligned(
    frames_in,
    ln1_gain,
    ln1_bias,
    qkv_weight,
    qv_bias,
    out_weight,
    out_bias,
    ln2_gain,
    ln2_bias,
    fc1_weight,
    fc1_bias,
    fc2_weight,
    fc2_bias,
    server_of_clip,
):
    dp, heads = lax.axis_size("dp"), lax.axis_size("head")
    groups, width = frames_in.shape[2], frames_in.shape[3] // 4
    frames, depth = groups * 4, width * heads
    rows = 16
    blocks = frames // (dp * rows)
    block = dp * rows
    columns, units = qkv_weight.shape[2], fc1_weight.shape[1]
    values = [
        ln1_gain, ln1_bias, ln2_gain, ln2_bias, qv_bias.reshape(-1), out_bias, fc2_bias, fc1_bias
    ]
    par = jnp.concatenate(values)[None]
    base = 4 * depth
    offsets = (
        (0, depth),
        (2 * depth, 3 * depth),
        base,
        base + columns,
        base + 2 * columns,
        base + 2 * columns + width,
        base + 2 * columns + 2 * width,
    )
    sizes = {
        "tile": 512,
        "chunk": 64,
        "offsets": offsets,
        "early": early,
        "later": later,
        "stages": (1, 5, 6, 7, 8),
    }
    bf16, f32 = jnp.bfloat16, jnp.float32
    dma = pltpu.SemaphoreType.DMA
    out = pl.pallas_call(
        functools.partial(layer_kernel, dp, sizes),
        out_shape=jax.ShapeDtypeStruct((groups, 4 * width), bf16),
        in_specs=[
            pl.BlockSpec(memory_space=pltpu.MemorySpace.SMEM),
            pl.BlockSpec(memory_space=VMEM),
        ]
        + [pl.BlockSpec(memory_space=ANY)] * 5,
        out_specs=pl.BlockSpec(memory_space=ANY),
        scratch_shapes=[
            pltpu.VMEM((3, depth, columns), bf16),
            pltpu.VMEM((heads, columns, width), bf16),
            pltpu.VMEM((depth, units), bf16),
            pltpu.VMEM((units, depth), bf16),
            pltpu.VMEM((frames, depth), bf16),
            pltpu.VMEM((frames, columns), bf16),
            pltpu.VMEM((frames, columns), bf16),
            pltpu.VMEM((frames, columns), bf16),
            pltpu.VMEM((frames, heads * columns), bf16),
            pltpu.VMEM((frames, width), bf16),
            pltpu.VMEM((blocks, dp, rows, width), bf16),
            pltpu.VMEM((frames, depth), bf16),
            pltpu.VMEM((block, depth), bf16),
            pltpu.VMEM((block, units), bf16),
            pltpu.VMEM((blocks, block, width), bf16),
            pltpu.VMEM((blocks, block, width), bf16),
            pltpu.VMEM((blocks, block, width), f32),
            pltpu.VMEM((frames, width), bf16),
            dma((4, 4, dp)),
            dma((4, dp)),
            dma((4,)),
            dma((4,)),
            dma((4,)),
            dma((4,)),
            dma,
            dma,
            dma((blocks,)),
            dma((blocks,)),
            dma((blocks, dp)),
            dma((blocks, dp)),
            dma((blocks, dp)),
            dma((blocks, dp)),
            dma((blocks,)),
            dma((blocks,)),
            dma((blocks,)),
            dma((blocks,)),
            dma((blocks, block // sizes["chunk"])),
        ]
        + [pltpu.VMEM((dp, rows, width), bf16)] * blocks,
        compiler_params=pltpu.CompilerParams(
            collective_id=0, has_side_effects=True, vmem_limit_bytes=66000000
        ),
        name="layer",
    )(
        slot_order(server_of_clip),
        par,
        frames_in[0, 0],
        jnp.swapaxes(qkv_weight, 0, 1),
        out_weight,
        fc1_weight,
        fc2_weight,
    )
    return out[None, None]


def aligned(mesh, frames_in, qkv_weight, out_weight, fc1_weight):
    dp, heads = mesh.shape["dp"], mesh.shape["head"]
    groups, width = frames_in.shape[2], frames_in.shape[3] // 4
    frames = groups * 4
    return (
        dp % 4 == 0
        and dp >= 16
        and heads == 2
        and frames % (dp * 16) == 0
        and groups % 64 == 0
        and (dp * 16) % 64 == 0
        and width % 128 == 0
        and out_weight.shape[0] % (dp * heads * 16) == 0
        and (qkv_weight.shape[2] // heads) % PAIR == 0
        and (qkv_weight.shape[0] // dp) % 16 == 0
        and (fc1_weight.shape[1] // heads) % 512 == 0
    )


def solution(mesh):
    placed = (
        P("dp", "head", None, None),
        P(),
        P(),
        P("dp", None, "head"),
        P(None, "head"),
        P(("head", "dp"), None),
        P("head"),
        P(),
        P(),
        P("dp", "head"),
        P("head"),
        P(("head", "dp"), None),
        P("head"),
        P(),
    )

    def layer(*args):
        body = on_device_aligned if aligned(mesh, args[0], args[3], args[5], args[9]) else on_device
        return jax.shard_map(
            body,
            mesh=mesh,
            in_specs=placed,
            out_specs=P("dp", "head", None, None),
            check_vma=False,
        )(*args)

    return layer
```

```python
import functools

import jax
import jax.numpy as jnp
from jax import lax
from jax.experimental import pallas as pl
from jax.experimental.pallas import tpu as pltpu
from jax.sharding import PartitionSpec as P

HDIM = 64


epsilon = 1e-05


def layer_norm(matrix, gain_row, shift_row):
    floats = matrix.astype(jnp.float32)
    center = jnp.mean(floats, axis=-1, keepdims=True)
    spread = jnp.mean(jnp.square(floats - center), axis=-1, keepdims=True)
    return ((floats - center) * lax.rsqrt(spread + epsilon) * gain_row + shift_row).astype(
        jnp.bfloat16
    )


def normalize(residual_in, gain_row, shift_row):
    whole_rows = lax.all_gather(residual_in, "head", axis=1, tiled=True)
    return layer_norm(whole_rows, gain_row, shift_row)


def attend(queries, key_rows, value_rows):

    def single(triple):
        query_head, key_head, value_head = triple
        scores = jnp.dot(query_head, key_head.T, preferred_element_type=jnp.float32)
        maxima = jnp.max(scores, axis=-1, keepdims=True)
        weights = jnp.exp(scores - maxima)
        probability = (weights / jnp.sum(weights, axis=-1, keepdims=True)).astype(jnp.bfloat16)
        return jnp.dot(probability, value_head, preferred_element_type=jnp.float32).astype(
            jnp.bfloat16
        )

    per_head = lax.map(
        single,
        (jnp.swapaxes(queries, 0, 1), jnp.swapaxes(key_rows, 0, 1), jnp.swapaxes(value_rows, 0, 1)),
    )
    return jnp.swapaxes(per_head, 0, 1).reshape(queries.shape[0], -1)


def slot_order(server_list):
    clip_count = server_list.shape[0]
    indices = jnp.arange(clip_count, dtype=jnp.int32)
    earlier = (server_list[None, :] < server_list[:, None]) | (
        server_list[None, :] == server_list[:, None]
    ) & (indices[None, :] < indices[:, None])
    slot_of = jnp.sum(earlier.astype(jnp.int32), axis=1)
    return jnp.sum(jnp.where(slot_of[None, :] == indices[:, None], indices[None, :], 0), axis=1)


def regroup(block_rows, clip_order):
    group_size = lax.axis_size("dp")
    piece_rows = block_rows.reshape(group_size, -1)
    shuffled = lax.all_to_all(piece_rows, "dp", split_axis=0, concat_axis=0, tiled=True)
    picked = jnp.take(shuffled, clip_order, axis=0)
    returned = lax.all_to_all(picked, "dp", split_axis=0, concat_axis=0, tiled=True)
    return returned.reshape(block_rows.shape)


def block_term(operand, weight_rows, row_count, frame_count, local_width):
    blocks = row_count // frame_count
    product = jnp.dot(operand, weight_rows, preferred_element_type=jnp.float32)
    return (
        product.reshape(frame_count, blocks, local_width)
        .transpose(1, 0, 2)
        .reshape(blocks * frame_count, local_width)
    )


def on_device(
    frames_in,
    ln1_gain,
    ln1_bias,
    qkv_weight,
    qv_bias,
    out_weight,
    out_bias,
    ln2_gain,
    ln2_bias,
    fc1_weight,
    fc1_bias,
    fc2_weight,
    fc2_bias,
    server_of_clip,
):
    clip_order = slot_order(server_of_clip)
    group_rows = frames_in.shape[2]
    local_width = frames_in.shape[3] // 4
    frame_count = group_rows * 4
    residual_in = frames_in[0, 0].reshape(frame_count, local_width)
    residual_in = regroup(residual_in, clip_order)
    normed_one = normalize(residual_in, ln1_gain, ln1_bias)
    column_count = qkv_weight.shape[2]
    weight_piece = lax.all_gather(qkv_weight, "dp", axis=0, tiled=True)
    operand = normed_one
    projected = jnp.dot(
        operand, weight_piece.reshape(weight_piece.shape[0], -1), preferred_element_type=jnp.float32
    ).reshape(frame_count, 3, column_count)
    queries = (
        ((projected[:, 0] + qv_bias[0]) * HDIM ** (-0.5))
        .astype(jnp.bfloat16)
        .reshape(frame_count, -1, HDIM)
    )
    key_rows = projected[:, 1].astype(jnp.bfloat16).reshape(frame_count, -1, HDIM)
    value_rows = (projected[:, 2] + qv_bias[1]).astype(jnp.bfloat16).reshape(frame_count, -1, HDIM)
    context = attend(queries, key_rows, value_rows)
    output_rows = lax.all_gather(out_weight, "dp", axis=0, tiled=True)
    carried = residual_in.astype(jnp.float32) + out_bias
    attended = (
        carried
        + lax.psum_scatter(
            block_term(
                context, output_rows, frame_count * lax.axis_size("head"), frame_count, local_width
            ).astype(jnp.bfloat16),
            "head",
            scatter_dimension=0,
            tiled=True,
        ).astype(jnp.float32)
    ).astype(jnp.bfloat16)
    normed_two = normalize(attended, ln2_gain, ln2_bias)
    operand = normed_two
    hidden_sums = jnp.dot(
        operand,
        lax.all_gather(fc1_weight, "dp", axis=0, tiled=True),
        preferred_element_type=jnp.float32,
    )
    hidden = jax.nn.gelu(hidden_sums + fc1_bias, approximate=False).astype(jnp.bfloat16)
    down_rows = lax.all_gather(fc2_weight, "dp", axis=0, tiled=True)
    kept = attended.astype(jnp.float32) + fc2_bias
    layer_out = (
        kept
        + lax.psum_scatter(
            block_term(
                hidden, down_rows, frame_count * lax.axis_size("head"), frame_count, local_width
            ).astype(jnp.bfloat16),
            "head",
            scatter_dimension=0,
            tiled=True,
        ).astype(jnp.float32)
    ).astype(jnp.bfloat16)
    return layer_out.reshape(1, 1, group_rows, 4 * local_width)


MESH = pl.DeviceIdType.MESH
VMEM = pltpu.MemorySpace.VMEM
ANY = pl.ANY
CORES = 2
PAIR = 2 * HDIM
UP, DOWN, SIDE, CORE = range(4)


def at_rows(index, rows):
    return pl.ds(pl.multiple_of(index * rows, rows), rows)


def norm_rows(floats, gain, shift):
    center = jnp.mean(floats, axis=-1, keepdims=True)
    moved = floats - center
    spread = jnp.mean(jnp.square(moved), axis=-1, keepdims=True)
    return (moved * lax.rsqrt(spread + epsilon) * gain + shift).astype(jnp.bfloat16)


def loop(start, stop, body):
    def step(k, carry):
        body(k)
        return carry

    lax.fori_loop(start, stop, step, 0)


class Gather:
    def __init__(self, me, h, dp, parts, send, recv):
        self.h, self.parts, self.send, self.recv = h, parts, send, recv
        self.sides = 2
        self.length = dp // (self.sides * CORES)
        self.core = lax.rem(me, CORES)
        self.side = lax.rem(lax.div(me, CORES), self.sides)
        self.z = lax.div(me, CORES * self.sides)
        self.started = []

    def index(self, z, side, core):
        return (z * self.sides + side) * CORES + core

    def copy(self, t, origin, route):
        target = {
            UP: lambda: self.index(self.z + 1, self.side, self.core),
            DOWN: lambda: self.index(self.z - 1, self.side, self.core),
            SIDE: lambda: self.index(self.z, 1 - self.side, self.core),
            CORE: lambda: self.index(self.z, self.side, 1 - self.core),
        }[route]()
        ref = self.parts[t](origin)
        return pltpu.make_async_remote_copy(
            ref, ref, self.send.at[t, route, origin], self.recv.at[t, origin], (target, self.h), MESH
        )

    def go(self, t, origin, routes, act):
        for route in routes:
            copy = self.copy(t, origin, route)
            if route == UP:
                pl.when(self.z < self.length - 1)(lambda copy=copy: act(copy))
            elif route == DOWN:
                pl.when(self.z > 0)(lambda copy=copy: act(copy))
            else:
                act(copy)

    def own(self, t, act, routes=(UP, DOWN, SIDE, CORE)):
        self.go(t, self.index(self.z, self.side, self.core), routes, act)

    def line(self, t, s, act, arrive=True):
        @pl.when(self.z >= s)
        def _():
            origin = self.index(self.z - s, self.side, self.core)
            if arrive:
                self.copy(t, origin, CORE).wait_recv()
            self.go(t, origin, (UP, SIDE, CORE), act)

        @pl.when(self.z + s < self.length)
        def _():
            origin = self.index(self.z + s, self.side, self.core)
            if arrive:
                self.copy(t, origin, CORE).wait_recv()
            self.go(t, origin, (DOWN, SIDE, CORE), act)

    def across(self, t, s, act, arrive=True):
        def one(z):
            origin = self.index(z, 1 - self.side, self.core)
            if arrive:
                self.copy(t, origin, CORE).wait_recv()
            self.go(t, origin, (CORE,), act)

        if s == 0:
            one(self.z)
            return
        pl.when(self.z >= s)(lambda: one(self.z - s))
        pl.when(self.z + s < self.length)(lambda: one(self.z + s))

    def twin(self, t, act, arrive=True):
        origin = self.index(self.z, 1 - self.side, self.core)
        if arrive:
            self.copy(t, origin, CORE).wait_recv()
        self.go(t, origin, (UP, DOWN, CORE), act)

    def both(self, t, s, act, arrive=True):
        def one(z, route):
            for side in range(self.sides):
                origin = self.index(z, side, self.core)
                if arrive:
                    self.copy(t, origin, CORE).wait_recv()
                self.go(t, origin, (route, CORE), act)

        pl.when(self.z >= s)(lambda: one(self.z - s, UP))
        pl.when(self.z + s < self.length)(lambda: one(self.z + s, DOWN))

    def rest(self, t):
        def one(k):
            origin = k * CORES + 1 - self.core
            self.copy(t, origin, CORE).wait_recv()

        loop(0, self.length * self.sides, one)

    def finish(self, t, paired):
        act = lambda copy: copy.wait_send()
        self.own(t, act)
        if paired:
            self.twin(t, act, False)
            for s in range(1, self.length):
                self.both(t, s, act, False)
            return
        for s in range(1, self.length):
            self.line(t, s, act, False)
        for s in range(self.length):
            self.across(t, s, act, False)


def layer_kernel(
    dp,
    sizes,
    order_ref,
    *refs,
):
    count = len(sizes["lengths"])
    values, refs = refs[:count], refs[count:]
    par_ref, par_sem, flat, refs = refs[-2 - count], refs[-1], refs[-1 - count : -1], refs[: -2 - count]
    copies = [
        pltpu.make_async_copy(value, part, par_sem.at[n])
        for n, (value, part) in enumerate(zip(values, flat))
    ]
    for copy in copies:
        copy.start()

    def fill():
        offset = 0
        for copy, part, length in zip(copies, flat, sizes["lengths"]):
            copy.wait()
            for row in range(part.shape[0] if len(part.shape) == 2 else 1):
                line = part[row : row + 1, :] if len(part.shape) == 2 else part[...][None, :]
                par_ref[0:1, offset : offset + length] = line
                offset += length

    layer_body(dp, sizes, order_ref, par_ref, fill, *refs)


def layer_body(
    dp,
    sizes,
    order_ref,
    par_ref,
    fill,
    x_ref,
    wq_ref,
    wo_ref,
    w1_ref,
    w2_ref,
    o_ref,
    all_q,
    all_o,
    all_1,
    all_2,
    x,
    q,
    k,
    v,
    ctx,
    att,
    second,
    full,
    normed,
    hidden,
    out,
    got,
    kept,
    done,
    placed,
    wsend,
    wrecv,
    own_sem,
    xs,
    xr,
    xo,
    os_,
    or_,
    cs,
    cr,
    s1,
    r1,
    s2,
    r2,
    s3,
    r3,
    fs,
    fr,
    ds,
):
    start = lambda copy: copy.start()
    me, h = lax.axis_index("dp"), lax.axis_index("head")
    there = 1 - h
    peer = (me, there)
    groups = x_ref.shape[0]
    width = x_ref.shape[1] // 4
    frames, depth = x.shape
    columns = q.shape[1]
    pairs = columns // PAIR
    blocks, _, rows, _ = second.shape
    block = frames // blocks
    tile = sizes["tile"]
    chunk = sizes["chunk"]
    (g1, b1), (g2, b2), qb, vb, ob, fb, f1 = sizes["offsets"]

    def par(offset, size):
        return par_ref[0:1, offset : offset + size]

    barrier = pltpu.get_barrier_semaphore()

    def hello(n):
        pl.semaphore_signal(barrier, inc=1, device_id=(lax.rem(me + n, dp), h), device_id_type=MESH)

    loop(1, dp, hello)
    pl.semaphore_signal(barrier, inc=1, device_id=peer, device_id_type=MESH)

    parts = [
        lambda d: all_q.at[:, at_rows(d, wq_ref.shape[1]), :],
        lambda d: all_o.at[:, at_rows(d, wo_ref.shape[0]), :],
        lambda d: all_1.at[at_rows(d, w1_ref.shape[0]), :],
        lambda d: all_2.at[at_rows(d, w2_ref.shape[0]), :],
    ]
    net = Gather(me, h, dp, parts, wsend, wrecv)
    mine = [
        pltpu.make_async_copy(wq_ref, parts[0](me), own_sem.at[0]),
        pltpu.make_async_copy(
            wo_ref.at[:, at_rows(h, width)],
            all_o.at[h, at_rows(me, wo_ref.shape[0]), :],
            own_sem.at[1],
        ),
        pltpu.make_async_copy(w1_ref, parts[2](me), own_sem.at[2]),
        pltpu.make_async_copy(w2_ref, parts[3](me), own_sem.at[3]),
    ]
    for copy in mine:
        copy.start()

    def x_part(j):
        return x_ref.at[:, j * width : (j + 1) * width], x.at[
            j * groups : (j + 1) * groups, at_rows(h, width)
        ]

    for j in range(4):
        pltpu.make_async_copy(*x_part(j), xo.at[j]).start()
    mine[0].wait()
    mine[2].wait()
    pl.semaphore_wait(barrier, dp)

    half = pltpu.make_async_remote_copy(
        wo_ref.at[:, at_rows(there, width)],
        all_o.at[h, at_rows(me, wo_ref.shape[0]), :],
        os_,
        or_,
        peer,
        MESH,
    )
    half.start()
    net.own(0, start)

    def x_copy(j):
        source, target = x_part(j)
        return pltpu.make_async_remote_copy(source, target, xs.at[j], xr.at[j], peer, MESH)

    for j in range(4):
        x_copy(j).start()

    def out_own():
        mine[1].wait()
        half.wait_recv()
        net.own(1, start)

    def out_twin():
        net.twin(1, start)

    def up_side():
        net.own(2, start, (SIDE,))

    def up_own():
        net.own(2, start, (UP, DOWN, CORE))

    def down_own():
        mine[3].wait()
        net.own(3, start, (UP, DOWN, CORE))

    def down_side():
        net.own(3, start, (SIDE,))

    L = lambda t, s: lambda: net.line(t, s, start)
    A = lambda t, s: lambda: net.across(t, s, start)
    B = lambda t, s: lambda: net.both(t, s, start)
    own = (out_own, out_twin, up_side, up_own, down_own, down_side)
    before, during, after = sizes["plan"](L, A, B, own)
    for n, step in enumerate(before):
        step()
        if n == 1:
            fill()
    net.rest(0)

    def project(j):
        at = at_rows(j, groups)
        n = norm_rows(x[at, :].astype(jnp.float32), par(g1, depth), par(b1, depth))

        def part(i):
            return jnp.dot(n, all_q[i], preferred_element_type=jnp.float32)

        q[at, :] = ((part(0) + par(qb, columns)) * HDIM ** (-0.5)).astype(jnp.bfloat16)
        k[at, :] = part(1).astype(jnp.bfloat16)
        v[at, :] = (part(2) + par(vb, columns)).astype(jnp.bfloat16)

    def x_wait(j):
        pltpu.make_async_copy(*x_part(j), xo.at[j]).wait()
        x_copy(j).wait_recv()

    def project_when_here(j):
        for n in range(4):
            pl.when(j == n)(lambda n=n: x_wait(n))
        project(j)

    loop(0, 4, project_when_here)

    lane = lax.broadcasted_iota(jnp.int32, (1, PAIR), 1)
    low_f = jnp.where(lane < HDIM, 1.0, 0.0)
    low, high = low_f.astype(jnp.bfloat16), (1.0 - low_f).astype(jnp.bfloat16)

    def attend(b, p):
        cols = at_rows(p, PAIR)
        keys, values = k[:, cols], v[:, cols]

        def head(query, value):
            scores = lax.dot_general(
                query, keys, (((1,), (1,)), ((), ())), preferred_element_type=jnp.float32
            )
            top = jnp.max(scores, axis=-1, keepdims=True)
            weights = jnp.exp(scores - top).astype(jnp.bfloat16)
            return jnp.dot(weights, value, preferred_element_type=jnp.float32)

        at = at_rows(b, block)
        query = q[at, cols]
        one = head(query * low, values * low + high)
        two = head(query * high, values * high + low)
        top = one * low_f + two * (1.0 - low_f)
        total = pltpu.roll(one * (1.0 - low_f) + two * low_f, HDIM, 1)
        ctx[at, at_rows(h * pairs + p, PAIR)] = (top / total).astype(jnp.bfloat16)

    def ctx_copy(b, p):
        ref = ctx.at[at_rows(b, block), at_rows(h * pairs + p, PAIR)]
        return pltpu.make_async_remote_copy(ref, ref, cs.at[b, p], cr.at[b, p], peer, MESH)

    def attended(b):
        loop(0, pairs, lambda p: ctx_copy(b, p).wait_recv())
        at = at_rows(b, block)
        total = x[at, at_rows(h, width)].astype(jnp.float32) + par(ob, width)
        for i in range(2):
            total = total + jnp.dot(
                ctx[at, i * columns : (i + 1) * columns],
                all_o[i],
                preferred_element_type=jnp.float32,
            )
        att[at, :] = total.astype(jnp.bfloat16)

    def piece(ref, b, j):
        return ref.at[at_rows(b * dp + j, rows)]

    def home(b, j):
        return full.at[at_rows(b * dp + j, rows), at_rows(h, width)]

    def one(b, n):
        other = lax.rem(me + n, dp)
        return pltpu.make_async_remote_copy(
            piece(att, b, other), home(b, me), s1.at[b, n], r1.at[b, n], (other, h), MESH
        )

    def one_own(b):
        return pltpu.make_async_copy(piece(att, b, me), home(b, me), r1.at[b, 0])

    def two(b, n):
        other = lax.rem(me + n, dp)
        return pltpu.make_async_remote_copy(
            second.at[b, other], piece(placed, b, me), s2.at[b, n], r2.at[b, n], (other, h), MESH
        )

    def two_own(b):
        return pltpu.make_async_copy(second.at[b, me], piece(placed, b, me), r2.at[b, 0])

    def three(b):
        ref = full.at[at_rows(b, block), at_rows(h, width)]
        return pltpu.make_async_remote_copy(ref, ref, s3.at[b], r3.at[b], peer, MESH)

    def spread(b):
        one_own(b).start()
        loop(1, dp, lambda n: one(b, n).start())

    def arrive(b):
        one_own(b).wait()
        loop(1, dp, lambda n: one(b, n).wait_recv())
        three(b).start()

    def share(target):
        return jnp.dot(
            hidden[...], all_2[:, at_rows(target, width)], preferred_element_type=jnp.float32
        )

    def out_copy(b):
        return pltpu.make_async_remote_copy(
            out.at[b], got.at[b], fs.at[b], fr.at[b], peer, MESH
        )

    def feed(b):
        three(b).wait_recv()
        at = at_rows(b, block)
        normed[...] = norm_rows(full[at, :].astype(jnp.float32), par(g2, depth), par(b2, depth))

        for t in range(hidden.shape[1] // tile):
            cols = slice(t * tile, (t + 1) * tile)
            sums = jnp.dot(normed[...], all_1[:, cols], preferred_element_type=jnp.float32)
            sums = sums + par(f1 + t * tile, tile)
            hidden[:, cols] = (0.5 * sums * (1.0 + lax.erf(sums * 0.7071067811865476))).astype(
                jnp.bfloat16
            )

        out[b] = share(there).astype(jnp.bfloat16)
        out_copy(b).start()
        kept[b] = full[at, at_rows(h, width)].astype(jnp.float32) + par(fb, width) + share(h)

    def done_copy(b, i):
        n = b * (block // chunk) + i
        per = groups // chunk
        return pltpu.make_async_copy(
            placed.at[at_rows(n, chunk)],
            o_ref.at[at_rows(lax.rem(n, per), chunk), at_rows(lax.div(n, per), width)],
            ds.at[b, i],
        )

    def close(b):
        out_copy(b).wait_recv()
        total = (kept[b] + got[b].astype(jnp.float32)).astype(jnp.bfloat16)
        done[...] = total.reshape(dp, rows, width)

        def choose(s):
            second[b, s] = done[order_ref[s]]

        loop(0, dp, choose)
        two_own(b).start()
        loop(1, dp, lambda n: two(b, n).start())

    def store(b):
        two_own(b).wait()
        loop(1, dp, lambda n: two(b, n).wait_recv())
        loop(0, block // chunk, lambda i: done_copy(b, i).start())

    def when(i, offset, body):
        b = i - offset

        @pl.when((b >= 0) & (b < blocks))
        def _():
            body(b)

    o_out, o_arrive, o_feed, o_close, o_store = sizes["stages"]

    def run(table, at):
        for n, steps in table.items():

            @pl.when(at == n)
            def _(steps=steps):
                for step in steps:
                    step()

    def master(i):
        def attend_block(b):
            def each(p):
                attend(b, p)
                ctx_copy(b, p).start()
                run(during, b * pairs + p)

            loop(0, pairs, each)

        when(i, 0, attend_block)

        def out_block(b):
            pl.when(b == 0)(lambda: net.rest(1))
            attended(b)
            spread(b)

        when(i, o_out, out_block)
        run(after, i)
        when(i, o_arrive, arrive)

        def feed_block(b):
            @pl.when(b == 0)
            def _():
                net.rest(2)
                net.rest(3)

            feed(b)

        when(i, o_feed, feed_block)
        when(i, o_close, close)
        when(i, o_store, store)

    loop(0, blocks + o_store, master)

    for t in range(4):
        net.finish(t, t == 1)
    half.wait_send()
    for j in range(4):
        x_copy(j).wait_send()

    def last(b):
        loop(0, pairs, lambda p: ctx_copy(b, p).wait_send())
        three(b).wait_send()
        out_copy(b).wait_send()
        loop(1, dp, lambda n: one(b, n).wait_send())
        loop(1, dp, lambda n: two(b, n).wait_send())
        loop(0, block // chunk, lambda i: done_copy(b, i).wait())

    loop(0, blocks, last)


def plan(L, A, B, own):
    out_own, out_twin, up_side, up_own, down_own, down_side = own
    before = [
        out_own, up_side, L(0, 1), out_twin, B(1, 1), L(0, 2), up_own, A(0, 0), A(0, 1), B(1, 2),
        L(0, 3), down_own, A(0, 2), B(1, 3), down_side, L(2, 1), A(0, 3),
    ]
    during = {0: [L(3, 1)], 8: [L(2, 2)], 14: [L(3, 2)]}
    after = {
        4: [L(2, 3)], 5: [L(3, 3), A(2, 0), A(3, 0), A(2, 1)], 6: [A(3, 1), A(2, 2)],
        7: [A(3, 2)], 8: [A(2, 3), A(3, 3)],
    }
    return before, during, after


def on_device_aligned(
    frames_in,
    ln1_gain,
    ln1_bias,
    qkv_weight,
    qv_bias,
    out_weight,
    out_bias,
    ln2_gain,
    ln2_bias,
    fc1_weight,
    fc1_bias,
    fc2_weight,
    fc2_bias,
    server_of_clip,
):
    dp, heads = lax.axis_size("dp"), lax.axis_size("head")
    groups, width = frames_in.shape[2], frames_in.shape[3] // 4
    frames, depth = groups * 4, width * heads
    rows = 16
    blocks = frames // (dp * rows)
    block = dp * rows
    columns, units = qkv_weight.shape[2], fc1_weight.shape[1]
    values = [
        ln1_gain, ln1_bias, ln2_gain, ln2_bias, qv_bias, out_bias, fc2_bias, fc1_bias
    ]
    base = 4 * depth
    offsets = (
        (0, depth),
        (2 * depth, 3 * depth),
        base,
        base + columns,
        base + 2 * columns,
        base + 2 * columns + width,
        base + 2 * columns + 2 * width,
    )
    sizes = {
        "tile": 512,
        "chunk": 64,
        "offsets": offsets,
        "lengths": [value.shape[-1] for value in values],
        "plan": plan,
        "stages": (1, 4, 8, 10, 12),
    }
    bf16, f32 = jnp.bfloat16, jnp.float32
    dma = pltpu.SemaphoreType.DMA
    out = pl.pallas_call(
        functools.partial(layer_kernel, dp, sizes),
        out_shape=jax.ShapeDtypeStruct((groups, 4 * width), bf16),
        in_specs=[
            pl.BlockSpec(memory_space=pltpu.MemorySpace.SMEM),
        ]
        + [pl.BlockSpec(memory_space=ANY)] * (5 + len(values)),
        out_specs=pl.BlockSpec(memory_space=ANY),
        scratch_shapes=[
            pltpu.VMEM((3, depth, columns), bf16),
            pltpu.VMEM((heads, columns, width), bf16),
            pltpu.VMEM((depth, units), bf16),
            pltpu.VMEM((units, depth), bf16),
            pltpu.VMEM((frames, depth), bf16),
            pltpu.VMEM((frames, columns), bf16),
            pltpu.VMEM((frames, columns), bf16),
            pltpu.VMEM((frames, columns), bf16),
            pltpu.VMEM((frames, heads * columns), bf16),
            pltpu.VMEM((frames, width), bf16),
            pltpu.VMEM((blocks, dp, rows, width), bf16),
            pltpu.VMEM((frames, depth), bf16),
            pltpu.VMEM((block, depth), bf16),
            pltpu.VMEM((block, units), bf16),
            pltpu.VMEM((blocks, block, width), bf16),
            pltpu.VMEM((blocks, block, width), bf16),
            pltpu.VMEM((blocks, block, width), f32),
            pltpu.VMEM((dp, rows, width), bf16),
            pltpu.VMEM((frames, width), bf16),
            dma((4, 4, dp)),
            dma((4, dp)),
            dma((4,)),
            dma((4,)),
            dma((4,)),
            dma((4,)),
            dma,
            dma,
            dma((blocks, columns // PAIR)),
            dma((blocks, columns // PAIR)),
            dma((blocks, dp)),
            dma((blocks, dp)),
            dma((blocks, dp)),
            dma((blocks, dp)),
            dma((blocks,)),
            dma((blocks,)),
            dma((blocks,)),
            dma((blocks,)),
            dma((blocks, block // sizes["chunk"])),
            pltpu.VMEM((1, sum(value.size for value in values)), f32),
            *[pltpu.VMEM(value.shape, f32) for value in values],
            dma((len(values),)),
        ],
        compiler_params=pltpu.CompilerParams(
            collective_id=0, has_side_effects=True, vmem_limit_bytes=66000000
        ),
        name="layer",
    )(
        slot_order(server_of_clip),
        *values,
        frames_in[0, 0],
        jnp.swapaxes(qkv_weight, 0, 1),
        out_weight,
        fc1_weight,
        fc2_weight,
    )
    return out[None, None]


def aligned(mesh, frames_in, qkv_weight, out_weight, fc1_weight):
    dp, heads = mesh.shape["dp"], mesh.shape["head"]
    groups, width = frames_in.shape[2], frames_in.shape[3] // 4
    frames = groups * 4
    return (
        dp % 4 == 0
        and dp >= 16
        and heads == 2
        and frames % (dp * 16) == 0
        and groups % 64 == 0
        and (dp * 16) % 64 == 0
        and width % 128 == 0
        and out_weight.shape[0] % (dp * heads * 16) == 0
        and (qkv_weight.shape[2] // heads) % PAIR == 0
        and (qkv_weight.shape[0] // dp) % 16 == 0
        and (fc1_weight.shape[1] // heads) % 512 == 0
    )


def solution(mesh):
    placed = (
        P("dp", "head", None, None),
        P(),
        P(),
        P("dp", None, "head"),
        P(None, "head"),
        P(("head", "dp"), None),
        P("head"),
        P(),
        P(),
        P("dp", "head"),
        P("head"),
        P(("head", "dp"), None),
        P("head"),
        P(),
    )

    def layer(*args):
        body = on_device_aligned if aligned(mesh, args[0], args[3], args[5], args[9]) else on_device
        return jax.shard_map(
            body,
            mesh=mesh,
            in_specs=placed,
            out_specs=P("dp", "head", None, None),
            check_vma=False,
        )(*args)

    return layer
```

```python
import functools

import jax
import jax.numpy as jnp
from jax import lax
from jax.experimental import pallas as pl
from jax.experimental.pallas import tpu as pltpu
from jax.sharding import PartitionSpec as P

HDIM = 64


epsilon = 1e-05


def layer_norm(matrix, gain_row, shift_row):
    floats = matrix.astype(jnp.float32)
    center = jnp.mean(floats, axis=-1, keepdims=True)
    spread = jnp.mean(jnp.square(floats - center), axis=-1, keepdims=True)
    return ((floats - center) * lax.rsqrt(spread + epsilon) * gain_row + shift_row).astype(
        jnp.bfloat16
    )


def normalize(residual_in, gain_row, shift_row):
    whole_rows = lax.all_gather(residual_in, "head", axis=1, tiled=True)
    return layer_norm(whole_rows, gain_row, shift_row)


def attend(queries, key_rows, value_rows):

    def single(triple):
        query_head, key_head, value_head = triple
        scores = jnp.dot(query_head, key_head.T, preferred_element_type=jnp.float32)
        maxima = jnp.max(scores, axis=-1, keepdims=True)
        weights = jnp.exp(scores - maxima)
        probability = (weights / jnp.sum(weights, axis=-1, keepdims=True)).astype(jnp.bfloat16)
        return jnp.dot(probability, value_head, preferred_element_type=jnp.float32).astype(
            jnp.bfloat16
        )

    per_head = lax.map(
        single,
        (jnp.swapaxes(queries, 0, 1), jnp.swapaxes(key_rows, 0, 1), jnp.swapaxes(value_rows, 0, 1)),
    )
    return jnp.swapaxes(per_head, 0, 1).reshape(queries.shape[0], -1)


def slot_order(server_list):
    clip_count = server_list.shape[0]
    indices = jnp.arange(clip_count, dtype=jnp.int32)
    earlier = (server_list[None, :] < server_list[:, None]) | (
        server_list[None, :] == server_list[:, None]
    ) & (indices[None, :] < indices[:, None])
    slot_of = jnp.sum(earlier.astype(jnp.int32), axis=1)
    return jnp.sum(jnp.where(slot_of[None, :] == indices[:, None], indices[None, :], 0), axis=1)


def regroup(block_rows, clip_order):
    group_size = lax.axis_size("dp")
    piece_rows = block_rows.reshape(group_size, -1)
    shuffled = lax.all_to_all(piece_rows, "dp", split_axis=0, concat_axis=0, tiled=True)
    picked = jnp.take(shuffled, clip_order, axis=0)
    returned = lax.all_to_all(picked, "dp", split_axis=0, concat_axis=0, tiled=True)
    return returned.reshape(block_rows.shape)


def block_term(operand, weight_rows, row_count, frame_count, local_width):
    blocks = row_count // frame_count
    product = jnp.dot(operand, weight_rows, preferred_element_type=jnp.float32)
    return (
        product.reshape(frame_count, blocks, local_width)
        .transpose(1, 0, 2)
        .reshape(blocks * frame_count, local_width)
    )


def on_device(
    frames_in,
    ln1_gain,
    ln1_bias,
    qkv_weight,
    qv_bias,
    out_weight,
    out_bias,
    ln2_gain,
    ln2_bias,
    fc1_weight,
    fc1_bias,
    fc2_weight,
    fc2_bias,
    server_of_clip,
):
    clip_order = slot_order(server_of_clip)
    group_rows = frames_in.shape[2]
    local_width = frames_in.shape[3] // 4
    frame_count = group_rows * 4
    residual_in = frames_in[0, 0].reshape(frame_count, local_width)
    residual_in = regroup(residual_in, clip_order)
    normed_one = normalize(residual_in, ln1_gain, ln1_bias)
    column_count = qkv_weight.shape[2]
    weight_piece = lax.all_gather(qkv_weight, "dp", axis=0, tiled=True)
    operand = normed_one
    projected = jnp.dot(
        operand, weight_piece.reshape(weight_piece.shape[0], -1), preferred_element_type=jnp.float32
    ).reshape(frame_count, 3, column_count)
    queries = (
        ((projected[:, 0] + qv_bias[0]) * HDIM ** (-0.5))
        .astype(jnp.bfloat16)
        .reshape(frame_count, -1, HDIM)
    )
    key_rows = projected[:, 1].astype(jnp.bfloat16).reshape(frame_count, -1, HDIM)
    value_rows = (projected[:, 2] + qv_bias[1]).astype(jnp.bfloat16).reshape(frame_count, -1, HDIM)
    context = attend(queries, key_rows, value_rows)
    output_rows = lax.all_gather(out_weight, "dp", axis=0, tiled=True)
    carried = residual_in.astype(jnp.float32) + out_bias
    attended = (
        carried
        + lax.psum_scatter(
            block_term(
                context, output_rows, frame_count * lax.axis_size("head"), frame_count, local_width
            ).astype(jnp.bfloat16),
            "head",
            scatter_dimension=0,
            tiled=True,
        ).astype(jnp.float32)
    ).astype(jnp.bfloat16)
    normed_two = normalize(attended, ln2_gain, ln2_bias)
    operand = normed_two
    hidden_sums = jnp.dot(
        operand,
        lax.all_gather(fc1_weight, "dp", axis=0, tiled=True),
        preferred_element_type=jnp.float32,
    )
    hidden = jax.nn.gelu(hidden_sums + fc1_bias, approximate=False).astype(jnp.bfloat16)
    down_rows = lax.all_gather(fc2_weight, "dp", axis=0, tiled=True)
    kept = attended.astype(jnp.float32) + fc2_bias
    layer_out = (
        kept
        + lax.psum_scatter(
            block_term(
                hidden, down_rows, frame_count * lax.axis_size("head"), frame_count, local_width
            ).astype(jnp.bfloat16),
            "head",
            scatter_dimension=0,
            tiled=True,
        ).astype(jnp.float32)
    ).astype(jnp.bfloat16)
    return layer_out.reshape(1, 1, group_rows, 4 * local_width)


MESH = pl.DeviceIdType.MESH
VMEM = pltpu.MemorySpace.VMEM
ANY = pl.ANY
CORES = 2
PAIR = 2 * HDIM
UP, DOWN, SIDE, CORE = range(4)


def at_rows(index, rows):
    return pl.ds(pl.multiple_of(index * rows, rows), rows)


def norm_rows(floats, gain, shift):
    center = jnp.mean(floats, axis=-1, keepdims=True)
    moved = floats - center
    spread = jnp.mean(jnp.square(moved), axis=-1, keepdims=True)
    return (moved * lax.rsqrt(spread + epsilon) * gain + shift).astype(jnp.bfloat16)


def loop(start, stop, body):
    def step(k, carry):
        body(k)
        return carry

    lax.fori_loop(start, stop, step, 0)


class Gather:
    def __init__(self, me, h, dp, parts, send, recv):
        self.h, self.parts, self.send, self.recv = h, parts, send, recv
        self.sides = 2
        self.length = dp // (self.sides * CORES)
        self.core = lax.rem(me, CORES)
        self.side = lax.rem(lax.div(me, CORES), self.sides)
        self.z = lax.div(me, CORES * self.sides)
        self.started = []

    def index(self, z, side, core):
        return (z * self.sides + side) * CORES + core

    def copy(self, t, origin, route):
        target = {
            UP: lambda: self.index(self.z + 1, self.side, self.core),
            DOWN: lambda: self.index(self.z - 1, self.side, self.core),
            SIDE: lambda: self.index(self.z, 1 - self.side, self.core),
            CORE: lambda: self.index(self.z, self.side, 1 - self.core),
        }[route]()
        ref = self.parts[t](origin)
        return pltpu.make_async_remote_copy(
            ref, ref, self.send.at[t, route, origin], self.recv.at[t, origin], (target, self.h), MESH
        )

    def go(self, t, origin, routes, act):
        for route in routes:
            copy = self.copy(t, origin, route)
            if route == UP:
                pl.when(self.z < self.length - 1)(lambda copy=copy: act(copy))
            elif route == DOWN:
                pl.when(self.z > 0)(lambda copy=copy: act(copy))
            else:
                act(copy)

    def own(self, t, act, routes=(UP, DOWN, SIDE, CORE)):
        self.go(t, self.index(self.z, self.side, self.core), routes, act)

    def line(self, t, s, act, arrive=True):
        @pl.when(self.z >= s)
        def _():
            origin = self.index(self.z - s, self.side, self.core)
            if arrive:
                self.copy(t, origin, CORE).wait_recv()
            self.go(t, origin, (UP, SIDE, CORE), act)

        @pl.when(self.z + s < self.length)
        def _():
            origin = self.index(self.z + s, self.side, self.core)
            if arrive:
                self.copy(t, origin, CORE).wait_recv()
            self.go(t, origin, (DOWN, SIDE, CORE), act)

    def across(self, t, s, act, arrive=True):
        def one(z):
            origin = self.index(z, 1 - self.side, self.core)
            if arrive:
                self.copy(t, origin, CORE).wait_recv()
            self.go(t, origin, (CORE,), act)

        if s == 0:
            one(self.z)
            return
        pl.when(self.z >= s)(lambda: one(self.z - s))
        pl.when(self.z + s < self.length)(lambda: one(self.z + s))

    def twin(self, t, act, arrive=True):
        origin = self.index(self.z, 1 - self.side, self.core)
        if arrive:
            self.copy(t, origin, CORE).wait_recv()
        self.go(t, origin, (UP, DOWN, CORE), act)

    def both(self, t, s, act, arrive=True):
        def one(z, route):
            for side in range(self.sides):
                origin = self.index(z, side, self.core)
                if arrive:
                    self.copy(t, origin, CORE).wait_recv()
                self.go(t, origin, (route, CORE), act)

        pl.when(self.z >= s)(lambda: one(self.z - s, UP))
        pl.when(self.z + s < self.length)(lambda: one(self.z + s, DOWN))

    def rest(self, t):
        def one(k):
            origin = k * CORES + 1 - self.core
            self.copy(t, origin, CORE).wait_recv()

        loop(0, self.length * self.sides, one)

    def finish(self, t, paired):
        act = lambda copy: copy.wait_send()
        self.own(t, act)
        if paired:
            self.twin(t, act, False)
            for s in range(1, self.length):
                self.both(t, s, act, False)
            return
        for s in range(1, self.length):
            self.line(t, s, act, False)
        for s in range(self.length):
            self.across(t, s, act, False)


def layer_kernel(
    dp,
    sizes,
    order_ref,
    *refs,
):
    count = len(sizes["lengths"])
    values, refs = refs[:count], refs[count:]
    par_ref, par_sem, flat, refs = refs[-2 - count], refs[-1], refs[-1 - count : -1], refs[: -2 - count]
    copies = [
        pltpu.make_async_copy(value, part, par_sem.at[n])
        for n, (value, part) in enumerate(zip(values, flat))
    ]
    for copy in copies:
        copy.start()

    def fill():
        offset = 0
        for copy, part, length in zip(copies, flat, sizes["lengths"]):
            copy.wait()
            for row in range(part.shape[0] if len(part.shape) == 2 else 1):
                line = part[row : row + 1, :] if len(part.shape) == 2 else part[...][None, :]
                par_ref[0:1, offset : offset + length] = line
                offset += length

    layer_body(dp, sizes, order_ref, par_ref, fill, *refs)


def layer_body(
    dp,
    sizes,
    order_ref,
    par_ref,
    fill,
    x_ref,
    wq_ref,
    wo_ref,
    w1_ref,
    w2_ref,
    o_ref,
    all_q,
    all_o,
    all_1,
    all_2,
    x,
    q,
    k,
    v,
    ctx,
    att,
    second,
    full,
    normed,
    hidden,
    out,
    got,
    done,
    placed,
    wsend,
    wrecv,
    own_sem,
    xs,
    xr,
    xo,
    os_,
    or_,
    cs,
    cr,
    s1,
    r1,
    s2,
    r2,
    s3,
    r3,
    fs,
    fr,
    ds,
):
    start = lambda copy: copy.start()
    me, h = lax.axis_index("dp"), lax.axis_index("head")
    there = 1 - h
    peer = (me, there)
    groups = x_ref.shape[0]
    width = x_ref.shape[1] // 4
    frames, depth = x.shape
    columns, units = q.shape[1], w1_ref.shape[1]
    pairs = columns // PAIR
    blocks, _, rows, _ = second.shape
    block = frames // blocks
    tile = sizes["tile"]
    chunk = sizes["chunk"]
    (g1, b1), (g2, b2), qb, vb, ob, fb, f1 = sizes["offsets"]

    def par(offset, size):
        return par_ref[0:1, offset : offset + size]

    barrier = pltpu.get_barrier_semaphore()

    def hello(n):
        pl.semaphore_signal(barrier, inc=1, device_id=(lax.rem(me + n, dp), h), device_id_type=MESH)

    loop(1, dp, hello)
    pl.semaphore_signal(barrier, inc=1, device_id=peer, device_id_type=MESH)

    parts = [
        lambda d: all_q.at[:, at_rows(d, wq_ref.shape[1]), :],
        lambda d: all_o.at[:, at_rows(d, wo_ref.shape[0]), :],
        lambda d: all_1.at[at_rows(d, w1_ref.shape[0]), : units // 2],
        lambda d: all_1.at[at_rows(d, w1_ref.shape[0]), units // 2 :],
        lambda d: all_2.at[at_rows(d, w2_ref.shape[0]), at_rows(there, width)],
        lambda d: all_2.at[at_rows(d, w2_ref.shape[0]), at_rows(h, width)],
    ]
    net = Gather(me, h, dp, parts, wsend, wrecv)
    mine = [
        pltpu.make_async_copy(wq_ref, parts[0](me), own_sem.at[0]),
        pltpu.make_async_copy(
            wo_ref.at[:, at_rows(h, width)],
            all_o.at[h, at_rows(me, wo_ref.shape[0]), :],
            own_sem.at[1],
        ),
        pltpu.make_async_copy(w1_ref, all_1.at[at_rows(me, w1_ref.shape[0]), :], own_sem.at[2]),
        pltpu.make_async_copy(w2_ref, all_2.at[at_rows(me, w2_ref.shape[0]), :], own_sem.at[3]),
    ]
    for copy in mine:
        copy.start()

    def x_part(j):
        return x_ref.at[:, j * width : (j + 1) * width], x.at[
            j * groups : (j + 1) * groups, at_rows(h, width)
        ]

    for j in range(4):
        pltpu.make_async_copy(*x_part(j), xo.at[j]).start()
    for n in (0, 2, 3):
        mine[n].wait()
    pl.semaphore_wait(barrier, dp)

    half = pltpu.make_async_remote_copy(
        wo_ref.at[:, at_rows(there, width)],
        all_o.at[h, at_rows(me, wo_ref.shape[0]), :],
        os_,
        or_,
        peer,
        MESH,
    )
    half.start()
    net.own(0, start)

    def x_copy(j):
        source, target = x_part(j)
        return pltpu.make_async_remote_copy(source, target, xs.at[j], xr.at[j], peer, MESH)

    for j in range(4):
        x_copy(j).start()

    def out_own():
        mine[1].wait()
        half.wait_recv()
        net.own(1, start)

    def out_twin():
        net.twin(1, start)

    L = lambda t, s: lambda: net.line(t, s, start)
    A = lambda t, s: lambda: net.across(t, s, start)
    B = lambda t, s: lambda: net.both(t, s, start)
    S = lambda t: lambda: net.own(t, start, (SIDE,))
    U = lambda t: lambda: net.own(t, start, (UP, DOWN, CORE))
    before, during, after = sizes["plan"](L, A, B, S, U, out_own, out_twin)
    for n, step in enumerate(before):
        step()
        if n == 1:
            fill()
    net.rest(0)

    def project(j):
        at = at_rows(j, groups)
        n = norm_rows(x[at, :].astype(jnp.float32), par(g1, depth), par(b1, depth))

        def part(i):
            return jnp.dot(n, all_q[i], preferred_element_type=jnp.float32)

        q[at, :] = ((part(0) + par(qb, columns)) * HDIM ** (-0.5)).astype(jnp.bfloat16)
        k[at, :] = part(1).astype(jnp.bfloat16)
        v[at, :] = (part(2) + par(vb, columns)).astype(jnp.bfloat16)

    def x_wait(j):
        pltpu.make_async_copy(*x_part(j), xo.at[j]).wait()
        x_copy(j).wait_recv()

    def project_when_here(j):
        for n in range(4):
            pl.when(j == n)(lambda n=n: x_wait(n))
        project(j)

    loop(0, 4, project_when_here)

    lane = lax.broadcasted_iota(jnp.int32, (1, PAIR), 1)
    low_f = jnp.where(lane < HDIM, 1.0, 0.0)
    low, high = low_f.astype(jnp.bfloat16), (1.0 - low_f).astype(jnp.bfloat16)

    def attend(b, p):
        cols = at_rows(p, PAIR)
        keys, values = k[:, cols], v[:, cols]

        def head(query, value):
            scores = lax.dot_general(
                query, keys, (((1,), (1,)), ((), ())), preferred_element_type=jnp.float32
            )
            top = jnp.max(scores, axis=-1, keepdims=True)
            weights = jnp.exp(scores - top).astype(jnp.bfloat16)
            return jnp.dot(weights, value, preferred_element_type=jnp.float32)

        at = at_rows(b, block)
        query = q[at, cols]
        one = head(query * low, values * low + high)
        two = head(query * high, values * high + low)
        top = one * low_f + two * (1.0 - low_f)
        total = pltpu.roll(one * (1.0 - low_f) + two * low_f, HDIM, 1)
        ctx[at, at_rows(h * pairs + p, PAIR)] = (top / total).astype(jnp.bfloat16)

    def ctx_copy(b, p):
        ref = ctx.at[at_rows(b, block), at_rows(h * pairs + p, PAIR)]
        return pltpu.make_async_remote_copy(ref, ref, cs.at[b, p], cr.at[b, p], peer, MESH)

    def attended(b):
        loop(0, pairs, lambda p: ctx_copy(b, p).wait_recv())
        at = at_rows(b, block)
        total = x[at, at_rows(h, width)].astype(jnp.float32) + par(ob, width)
        for i in range(2):
            total = total + jnp.dot(
                ctx[at, i * columns : (i + 1) * columns],
                all_o[i],
                preferred_element_type=jnp.float32,
            )
        att[at, :] = total.astype(jnp.bfloat16)

    def piece(ref, b, j):
        return ref.at[at_rows(b * dp + j, rows)]

    def home(b, j):
        return full.at[at_rows(b * dp + j, rows), at_rows(h, width)]

    def one(b, n):
        other = lax.rem(me + n, dp)
        return pltpu.make_async_remote_copy(
            piece(att, b, other), home(b, me), s1.at[b, n], r1.at[b, n], (other, h), MESH
        )

    def one_own(b):
        return pltpu.make_async_copy(piece(att, b, me), home(b, me), r1.at[b, 0])

    def two(b, n):
        other = lax.rem(me + n, dp)
        return pltpu.make_async_remote_copy(
            second.at[b, other], piece(placed, b, me), s2.at[b, n], r2.at[b, n], (other, h), MESH
        )

    def two_own(b):
        return pltpu.make_async_copy(second.at[b, me], piece(placed, b, me), r2.at[b, 0])

    def three(b):
        ref = full.at[at_rows(b, block), at_rows(h, width)]
        return pltpu.make_async_remote_copy(ref, ref, s3.at[b], r3.at[b], peer, MESH)

    def spread(b):
        one_own(b).start()
        loop(1, dp, lambda n: one(b, n).start())

    def arrive(b):
        one_own(b).wait()
        loop(1, dp, lambda n: one(b, n).wait_recv())
        three(b).start()

    def share(b, target):
        return jnp.dot(
            hidden[at_rows(b, block), :],
            all_2[:, at_rows(target, width)],
            preferred_element_type=jnp.float32,
        )

    def out_copy(b):
        return pltpu.make_async_remote_copy(
            out.at[b], got.at[b], fs.at[b], fr.at[b], peer, MESH
        )

    def feed(b):
        three(b).wait_recv()
        at = at_rows(b, block)
        normed[...] = norm_rows(full[at, :].astype(jnp.float32), par(g2, depth), par(b2, depth))

        for t in range(units // tile):
            cols = slice(t * tile, (t + 1) * tile)
            sums = jnp.dot(normed[...], all_1[:, cols], preferred_element_type=jnp.float32)
            sums = sums + par(f1 + t * tile, tile)
            hidden[at, cols] = (0.5 * sums * (1.0 + lax.erf(sums * 0.7071067811865476))).astype(
                jnp.bfloat16
            )

        out[b] = share(b, there).astype(jnp.bfloat16)
        out_copy(b).start()

    def done_copy(b, i):
        n = b * (block // chunk) + i
        per = groups // chunk
        return pltpu.make_async_copy(
            placed.at[at_rows(n, chunk)],
            o_ref.at[at_rows(lax.rem(n, per), chunk), at_rows(lax.div(n, per), width)],
            ds.at[b, i],
        )

    def close(b):
        at = at_rows(b, block)
        kept = full[at, at_rows(h, width)].astype(jnp.float32) + par(fb, width) + share(b, h)
        out_copy(b).wait_recv()
        total = (kept + got[b].astype(jnp.float32)).astype(jnp.bfloat16)
        done[...] = total.reshape(dp, rows, width)

        def choose(s):
            second[b, s] = done[order_ref[s]]

        loop(0, dp, choose)
        two_own(b).start()
        loop(1, dp, lambda n: two(b, n).start())

    def store(b):
        two_own(b).wait()
        loop(1, dp, lambda n: two(b, n).wait_recv())
        loop(0, block // chunk, lambda i: done_copy(b, i).start())

    def when(i, offset, body):
        b = i - offset

        @pl.when((b >= 0) & (b < blocks))
        def _():
            body(b)

    o_arrive, o_feed, o_close, o_store = sizes["stages"]

    def run(table, at):
        for n, steps in table.items():

            @pl.when(at == n)
            def _(steps=steps):
                for step in steps:
                    step()

    def sent():
        half.wait_send()
        for j in range(4):
            x_copy(j).wait_send()

        def block_sent(b):
            loop(0, pairs, lambda p: ctx_copy(b, p).wait_send())
            loop(1, dp, lambda n: one(b, n).wait_send())

        loop(0, blocks, block_sent)
        for t in range(5):
            net.finish(t, t == 1)

    def master(i):
        def out_block(b):
            pl.when(b == 0)(lambda: net.rest(1))
            attended(b)
            spread(b)

        def attend_block(b):
            def each(p):
                attend(b, p)
                ctx_copy(b, p).start()
                pl.when((p == 1) & (b > 0))(lambda: out_block(b - 1))
                run(during, b * pairs + p)

            loop(0, pairs, each)

        when(i, 0, attend_block)
        pl.when(i == blocks)(lambda: out_block(blocks - 1))
        run(after, i)
        when(i, o_arrive, arrive)

        def feed_block(b):
            @pl.when(b == 0)
            def _():
                for t in (2, 3, 4):
                    net.rest(t)

            feed(b)

        when(i, o_feed, feed_block)

        def close_block(b):
            pl.when(b == 0)(lambda: net.rest(5))
            close(b)
            pl.when(b == 0)(sent)
            pl.when(b == 1)(lambda: net.finish(5, False))

        when(i, o_close, close_block)
        when(i, o_store, store)

    loop(0, blocks + o_store, master)

    def last(b):
        three(b).wait_send()
        out_copy(b).wait_send()
        loop(1, dp, lambda n: two(b, n).wait_send())
        loop(0, block // chunk, lambda i: done_copy(b, i).wait())

    loop(0, blocks, last)


def plan(L, A, B, S, U, out_own, out_twin):
    before = [
        out_own, S(2), L(0, 1), out_twin, B(1, 1), U(2), L(0, 2), S(3), A(0, 0), A(0, 1), B(1, 2),
        U(3), L(0, 3), S(4), U(4), A(0, 2), L(2, 1), A(0, 3),
    ]
    during = {
        0: [L(3, 1)], 1: [B(1, 3)], 2: [L(4, 1)], 6: [L(2, 2)], 10: [L(3, 2)], 14: [L(4, 2)],
        18: [L(2, 3)],
    }
    after = {
        4: [S(5), U(5)], 5: [L(3, 3), A(2, 0), A(3, 0), A(4, 0), A(2, 1), A(3, 1), A(4, 1)],
        6: [L(4, 3), L(5, 1), A(2, 2), A(3, 2), A(4, 2), A(2, 3), A(3, 3)], 7: [L(5, 2), A(4, 3)],
        8: [L(5, 3), A(5, 0)], 9: [A(5, 1)], 10: [A(5, 2)], 11: [A(5, 3)],
    }
    return before, during, after


def on_device_aligned(
    frames_in,
    ln1_gain,
    ln1_bias,
    qkv_weight,
    qv_bias,
    out_weight,
    out_bias,
    ln2_gain,
    ln2_bias,
    fc1_weight,
    fc1_bias,
    fc2_weight,
    fc2_bias,
    server_of_clip,
):
    dp, heads = lax.axis_size("dp"), lax.axis_size("head")
    groups, width = frames_in.shape[2], frames_in.shape[3] // 4
    frames, depth = groups * 4, width * heads
    rows = 16
    blocks = frames // (dp * rows)
    block = dp * rows
    columns, units = qkv_weight.shape[2], fc1_weight.shape[1]
    values = [
        ln1_gain, ln1_bias, ln2_gain, ln2_bias, qv_bias, out_bias, fc2_bias, fc1_bias
    ]
    base = 4 * depth
    offsets = (
        (0, depth),
        (2 * depth, 3 * depth),
        base,
        base + columns,
        base + 2 * columns,
        base + 2 * columns + width,
        base + 2 * columns + 2 * width,
    )
    sizes = {
        "tile": 512,
        "chunk": 64,
        "offsets": offsets,
        "lengths": [value.shape[-1] for value in values],
        "plan": plan,
        "stages": (2, 7, 12, 14),
    }
    bf16, f32 = jnp.bfloat16, jnp.float32
    dma = pltpu.SemaphoreType.DMA
    out = pl.pallas_call(
        functools.partial(layer_kernel, dp, sizes),
        out_shape=jax.ShapeDtypeStruct((groups, 4 * width), bf16),
        in_specs=[
            pl.BlockSpec(memory_space=pltpu.MemorySpace.SMEM),
        ]
        + [pl.BlockSpec(memory_space=ANY)] * (5 + len(values)),
        out_specs=pl.BlockSpec(memory_space=ANY),
        scratch_shapes=[
            pltpu.VMEM((3, depth, columns), bf16),
            pltpu.VMEM((heads, columns, width), bf16),
            pltpu.VMEM((depth, units), bf16),
            pltpu.VMEM((units, depth), bf16),
            pltpu.VMEM((frames, depth), bf16),
            pltpu.VMEM((frames, columns), bf16),
            pltpu.VMEM((frames, columns), bf16),
            pltpu.VMEM((frames, columns), bf16),
            pltpu.VMEM((frames, heads * columns), bf16),
            pltpu.VMEM((frames, width), bf16),
            pltpu.VMEM((blocks, dp, rows, width), bf16),
            pltpu.VMEM((frames, depth), bf16),
            pltpu.VMEM((block, depth), bf16),
            pltpu.VMEM((frames, units), bf16),
            pltpu.VMEM((blocks, block, width), bf16),
            pltpu.VMEM((blocks, block, width), bf16),
            pltpu.VMEM((dp, rows, width), bf16),
            pltpu.VMEM((frames, width), bf16),
            dma((6, 4, dp)),
            dma((6, dp)),
            dma((4,)),
            dma((4,)),
            dma((4,)),
            dma((4,)),
            dma,
            dma,
            dma((blocks, columns // PAIR)),
            dma((blocks, columns // PAIR)),
            dma((blocks, dp)),
            dma((blocks, dp)),
            dma((blocks, dp)),
            dma((blocks, dp)),
            dma((blocks,)),
            dma((blocks,)),
            dma((blocks,)),
            dma((blocks,)),
            dma((blocks, block // sizes["chunk"])),
            pltpu.VMEM((1, sum(value.size for value in values)), f32),
            *[pltpu.VMEM(value.shape, f32) for value in values],
            dma((len(values),)),
        ],
        compiler_params=pltpu.CompilerParams(
            collective_id=0, has_side_effects=True, vmem_limit_bytes=66000000
        ),
        name="layer",
    )(
        slot_order(server_of_clip),
        *values,
        frames_in[0, 0],
        jnp.swapaxes(qkv_weight, 0, 1),
        out_weight,
        fc1_weight,
        fc2_weight,
    )
    return out[None, None]


def aligned(mesh, frames_in, qkv_weight, out_weight, fc1_weight):
    dp, heads = mesh.shape["dp"], mesh.shape["head"]
    groups, width = frames_in.shape[2], frames_in.shape[3] // 4
    frames = groups * 4
    return (
        dp % 4 == 0
        and dp >= 16
        and heads == 2
        and frames % (dp * 16) == 0
        and groups % 64 == 0
        and (dp * 16) % 64 == 0
        and width % 128 == 0
        and out_weight.shape[0] % (dp * heads * 16) == 0
        and (qkv_weight.shape[2] // heads) % PAIR == 0
        and (qkv_weight.shape[0] // dp) % 16 == 0
        and (fc1_weight.shape[1] // heads) % 512 == 0
    )


def solution(mesh):
    placed = (
        P("dp", "head", None, None),
        P(),
        P(),
        P("dp", None, "head"),
        P(None, "head"),
        P(("head", "dp"), None),
        P("head"),
        P(),
        P(),
        P("dp", "head"),
        P("head"),
        P(("head", "dp"), None),
        P("head"),
        P(),
    )

    def layer(*args):
        body = on_device_aligned if aligned(mesh, args[0], args[3], args[5], args[9]) else on_device
        return jax.shard_map(
            body,
            mesh=mesh,
            in_specs=placed,
            out_specs=P("dp", "head", None, None),
            check_vma=False,
        )(*args)

    return layer
```

```python
import functools

import jax
import jax.numpy as jnp
from jax import lax
from jax.experimental import pallas as pl
from jax.experimental.pallas import tpu as pltpu
from jax.sharding import PartitionSpec as P

HDIM = 64


epsilon = 1e-05


def layer_norm(matrix, gain_row, shift_row):
    floats = matrix.astype(jnp.float32)
    center = jnp.mean(floats, axis=-1, keepdims=True)
    spread = jnp.mean(jnp.square(floats - center), axis=-1, keepdims=True)
    return ((floats - center) * lax.rsqrt(spread + epsilon) * gain_row + shift_row).astype(
        jnp.bfloat16
    )


def normalize(residual_in, gain_row, shift_row):
    whole_rows = lax.all_gather(residual_in, "head", axis=1, tiled=True)
    return layer_norm(whole_rows, gain_row, shift_row)


def attend(queries, key_rows, value_rows):

    def single(triple):
        query_head, key_head, value_head = triple
        scores = jnp.dot(query_head, key_head.T, preferred_element_type=jnp.float32)
        maxima = jnp.max(scores, axis=-1, keepdims=True)
        weights = jnp.exp(scores - maxima)
        probability = (weights / jnp.sum(weights, axis=-1, keepdims=True)).astype(jnp.bfloat16)
        return jnp.dot(probability, value_head, preferred_element_type=jnp.float32).astype(
            jnp.bfloat16
        )

    per_head = lax.map(
        single,
        (jnp.swapaxes(queries, 0, 1), jnp.swapaxes(key_rows, 0, 1), jnp.swapaxes(value_rows, 0, 1)),
    )
    return jnp.swapaxes(per_head, 0, 1).reshape(queries.shape[0], -1)


def slot_order(server_list):
    clip_count = server_list.shape[0]
    indices = jnp.arange(clip_count, dtype=jnp.int32)
    earlier = (server_list[None, :] < server_list[:, None]) | (
        server_list[None, :] == server_list[:, None]
    ) & (indices[None, :] < indices[:, None])
    slot_of = jnp.sum(earlier.astype(jnp.int32), axis=1)
    return jnp.sum(jnp.where(slot_of[None, :] == indices[:, None], indices[None, :], 0), axis=1)


def regroup(block_rows, clip_order):
    group_size = lax.axis_size("dp")
    piece_rows = block_rows.reshape(group_size, -1)
    shuffled = lax.all_to_all(piece_rows, "dp", split_axis=0, concat_axis=0, tiled=True)
    picked = jnp.take(shuffled, clip_order, axis=0)
    returned = lax.all_to_all(picked, "dp", split_axis=0, concat_axis=0, tiled=True)
    return returned.reshape(block_rows.shape)


def block_term(operand, weight_rows, row_count, frame_count, local_width):
    blocks = row_count // frame_count
    product = jnp.dot(operand, weight_rows, preferred_element_type=jnp.float32)
    return (
        product.reshape(frame_count, blocks, local_width)
        .transpose(1, 0, 2)
        .reshape(blocks * frame_count, local_width)
    )


def on_device(
    frames_in,
    ln1_gain,
    ln1_bias,
    qkv_weight,
    qv_bias,
    out_weight,
    out_bias,
    ln2_gain,
    ln2_bias,
    fc1_weight,
    fc1_bias,
    fc2_weight,
    fc2_bias,
    server_of_clip,
):
    clip_order = slot_order(server_of_clip)
    group_rows = frames_in.shape[2]
    local_width = frames_in.shape[3] // 4
    frame_count = group_rows * 4
    residual_in = frames_in[0, 0].reshape(frame_count, local_width)
    residual_in = regroup(residual_in, clip_order)
    normed_one = normalize(residual_in, ln1_gain, ln1_bias)
    column_count = qkv_weight.shape[2]
    weight_piece = lax.all_gather(qkv_weight, "dp", axis=0, tiled=True)
    operand = normed_one
    projected = jnp.dot(
        operand, weight_piece.reshape(weight_piece.shape[0], -1), preferred_element_type=jnp.float32
    ).reshape(frame_count, 3, column_count)
    queries = (
        ((projected[:, 0] + qv_bias[0]) * HDIM ** (-0.5))
        .astype(jnp.bfloat16)
        .reshape(frame_count, -1, HDIM)
    )
    key_rows = projected[:, 1].astype(jnp.bfloat16).reshape(frame_count, -1, HDIM)
    value_rows = (projected[:, 2] + qv_bias[1]).astype(jnp.bfloat16).reshape(frame_count, -1, HDIM)
    context = attend(queries, key_rows, value_rows)
    output_rows = lax.all_gather(out_weight, "dp", axis=0, tiled=True)
    carried = residual_in.astype(jnp.float32) + out_bias
    attended = (
        carried
        + lax.psum_scatter(
            block_term(
                context, output_rows, frame_count * lax.axis_size("head"), frame_count, local_width
            ).astype(jnp.bfloat16),
            "head",
            scatter_dimension=0,
            tiled=True,
        ).astype(jnp.float32)
    ).astype(jnp.bfloat16)
    normed_two = normalize(attended, ln2_gain, ln2_bias)
    operand = normed_two
    hidden_sums = jnp.dot(
        operand,
        lax.all_gather(fc1_weight, "dp", axis=0, tiled=True),
        preferred_element_type=jnp.float32,
    )
    hidden = jax.nn.gelu(hidden_sums + fc1_bias, approximate=False).astype(jnp.bfloat16)
    down_rows = lax.all_gather(fc2_weight, "dp", axis=0, tiled=True)
    kept = attended.astype(jnp.float32) + fc2_bias
    layer_out = (
        kept
        + lax.psum_scatter(
            block_term(
                hidden, down_rows, frame_count * lax.axis_size("head"), frame_count, local_width
            ).astype(jnp.bfloat16),
            "head",
            scatter_dimension=0,
            tiled=True,
        ).astype(jnp.float32)
    ).astype(jnp.bfloat16)
    return layer_out.reshape(1, 1, group_rows, 4 * local_width)


MESH = pl.DeviceIdType.MESH
VMEM = pltpu.MemorySpace.VMEM
ANY = pl.ANY
CORES = 2
PAIR = 2 * HDIM
UP, DOWN, SIDE, CORE = range(4)


def at_rows(index, rows):
    return pl.ds(pl.multiple_of(index * rows, rows), rows)


def norm_rows(floats, gain, shift):
    center = jnp.mean(floats, axis=-1, keepdims=True)
    moved = floats - center
    spread = jnp.mean(jnp.square(moved), axis=-1, keepdims=True)
    return (moved * lax.rsqrt(spread + epsilon) * gain + shift).astype(jnp.bfloat16)


def loop(start, stop, body):
    def step(k, carry):
        body(k)
        return carry

    lax.fori_loop(start, stop, step, 0)


class Gather:
    def __init__(self, me, h, dp, parts, send, recv, near):
        self.h, self.parts, self.send, self.recv, self.near = h, parts, send, recv, near
        self.sides = 2
        self.length = dp // (self.sides * CORES)
        self.core = lax.rem(me, CORES)
        self.side = lax.rem(lax.div(me, CORES), self.sides)
        self.z = lax.div(me, CORES * self.sides)

    def index(self, z, side, core):
        return (z * self.sides + side) * CORES + core

    def copy(self, t, origin, route, count=1):
        target = {
            UP: lambda: self.index(self.z + 1, self.side, self.core),
            DOWN: lambda: self.index(self.z - 1, self.side, self.core),
            SIDE: lambda: self.index(self.z, 1 - self.side, self.core),
            CORE: lambda: self.index(self.z, self.side, 1 - self.core),
        }[route]()
        ref = self.parts[t](origin, count)
        near = self.near.at[t] if route == CORE else self.recv.at[t, lax.div(origin, CORES)]
        return pltpu.make_async_remote_copy(
            ref, ref, self.send.at[t, route], near, (target, self.h), MESH
        )

    def go(self, t, origin, routes, act):
        for route in routes:
            copy = self.copy(t, origin, route)
            if route == UP:
                pl.when(self.z < self.length - 1)(lambda copy=copy: act(copy))
            elif route == DOWN:
                pl.when(self.z > 0)(lambda copy=copy: act(copy))
            else:
                act(copy)

    def own(self, t, act, routes=(UP, DOWN, SIDE, CORE)):
        self.go(t, self.index(self.z, self.side, self.core), routes, act)

    def line(self, t, s, act):
        @pl.when(self.z >= s)
        def _():
            origin = self.index(self.z - s, self.side, self.core)
            self.copy(t, origin, SIDE).wait_recv()
            self.go(t, origin, (UP, SIDE, CORE), act)

        @pl.when(self.z + s < self.length)
        def _():
            origin = self.index(self.z + s, self.side, self.core)
            self.copy(t, origin, SIDE).wait_recv()
            self.go(t, origin, (DOWN, SIDE, CORE), act)

    def across(self, t, s, act):
        def one(z):
            origin = self.index(z, 1 - self.side, self.core)
            self.copy(t, origin, SIDE).wait_recv()
            self.go(t, origin, (CORE,), act)

        if s == 0:
            one(self.z)
            return
        pl.when(self.z >= s)(lambda: one(self.z - s))
        pl.when(self.z + s < self.length)(lambda: one(self.z + s))

    def twin(self, t, act):
        origin = self.index(self.z, 1 - self.side, self.core)
        self.copy(t, origin, SIDE).wait_recv()
        self.go(t, origin, (UP, DOWN, CORE), act)

    def both(self, t, s, act):
        def one(z, route):
            for side in range(self.sides):
                origin = self.index(z, side, self.core)
                self.copy(t, origin, SIDE).wait_recv()
                self.go(t, origin, (route, CORE), act)

        pl.when(self.z >= s)(lambda: one(self.z - s, UP))
        pl.when(self.z + s < self.length)(lambda: one(self.z + s, DOWN))

    def rest(self, t):
        self.copy(t, 0, CORE, self.length * self.sides).wait_recv()

    def finish(self, t, paired):
        each = self.sides if paired else 1
        self.copy(t, 0, CORE, self.length * self.sides).wait_send()
        self.copy(t, 0, SIDE, 1 if paired else self.length).wait_send()
        for z in range(self.length - 1):
            up = self.copy(t, 0, UP, (z + 1) * each)
            pl.when(self.z == z)(lambda copy=up: copy.wait_send())
            down = self.copy(t, 0, DOWN, (z + 1) * each)
            pl.when(self.z == self.length - 1 - z)(lambda copy=down: copy.wait_send())


def layer_kernel(
    dp,
    sizes,
    order_ref,
    *refs,
):
    count = len(sizes["lengths"])
    values, refs = refs[:count], refs[count:]
    par_ref, par_sem, flat, refs = refs[-2 - count], refs[-1], refs[-1 - count : -1], refs[: -2 - count]
    copies = [
        pltpu.make_async_copy(value, part, par_sem.at[n])
        for n, (value, part) in enumerate(zip(values, flat))
    ]
    for copy in copies:
        copy.start()

    def fill():
        offset = 0
        for copy, part, length in zip(copies, flat, sizes["lengths"]):
            copy.wait()
            for row in range(part.shape[0] if len(part.shape) == 2 else 1):
                line = part[row : row + 1, :] if len(part.shape) == 2 else part[...][None, :]
                par_ref[0:1, offset : offset + length] = line
                offset += length

    layer_body(dp, sizes, order_ref, par_ref, fill, *refs)


def layer_body(
    dp,
    sizes,
    order_ref,
    par_ref,
    fill,
    x_ref,
    wq_ref,
    wo_ref,
    w1_ref,
    w2_ref,
    o_ref,
    all_q,
    all_o,
    all_1,
    all_2,
    x,
    q,
    k,
    v,
    ctx,
    att,
    second,
    full,
    normed,
    hidden,
    out,
    got,
    done,
    placed,
    wsend,
    wrecv,
    wnear,
    own_sem,
    xs,
    xr,
    xo,
    os_,
    or_,
    cs,
    cr,
    s1,
    r1,
    l1,
    s2,
    r2,
    l2,
    s3,
    r3,
    fs,
    fr,
    ds,
):
    start = lambda copy: copy.start()
    me, h = lax.axis_index("dp"), lax.axis_index("head")
    there = 1 - h
    peer = (me, there)
    groups = x_ref.shape[0]
    width = x_ref.shape[1] // 4
    frames, depth = x.shape
    columns, units = q.shape[1], w1_ref.shape[1]
    pairs = columns // PAIR
    blocks, _, rows, _ = second.shape
    block = frames // blocks
    tile = sizes["tile"]
    chunk = sizes["chunk"]
    (g1, b1), (g2, b2), qb, vb, ob, fb, f1 = sizes["offsets"]

    def par(offset, size):
        return par_ref[0:1, offset : offset + size]

    barrier = pltpu.get_barrier_semaphore()

    def hello(n):
        pl.semaphore_signal(barrier, inc=1, device_id=(lax.rem(me + n, dp), h), device_id_type=MESH)

    loop(1, dp, hello)
    pl.semaphore_signal(barrier, inc=1, device_id=peer, device_id_type=MESH)

    def span(d, rows, count):
        return pl.ds(pl.multiple_of(d * rows, rows), rows * count)

    parts = [
        lambda d, n=1: all_q.at[:, span(d, wq_ref.shape[1], n), :],
        lambda d, n=1: all_o.at[:, span(d, wo_ref.shape[0], n), :],
        lambda d, n=1: all_1.at[span(d, w1_ref.shape[0], n), : units // 2],
        lambda d, n=1: all_1.at[span(d, w1_ref.shape[0], n), units // 2 :],
        lambda d, n=1: all_2.at[span(d, w2_ref.shape[0], n), at_rows(there, width)],
        lambda d, n=1: all_2.at[span(d, w2_ref.shape[0], n), at_rows(h, width)],
    ]
    net = Gather(me, h, dp, parts, wsend, wrecv, wnear)
    mine = [
        pltpu.make_async_copy(wq_ref, parts[0](me), own_sem.at[0]),
        pltpu.make_async_copy(
            wo_ref.at[:, at_rows(h, width)],
            all_o.at[h, at_rows(me, wo_ref.shape[0]), :],
            own_sem.at[1],
        ),
        pltpu.make_async_copy(w1_ref, all_1.at[at_rows(me, w1_ref.shape[0]), :], own_sem.at[2]),
        pltpu.make_async_copy(w2_ref, all_2.at[at_rows(me, w2_ref.shape[0]), :], own_sem.at[3]),
    ]
    for copy in mine:
        copy.start()

    def x_part(j):
        return x_ref.at[:, j * width : (j + 1) * width], x.at[
            j * groups : (j + 1) * groups, at_rows(h, width)
        ]

    for j in range(4):
        pltpu.make_async_copy(*x_part(j), xo.at[j]).start()
    for n in (0, 2, 3):
        mine[n].wait()
    pl.semaphore_wait(barrier, dp)

    half = pltpu.make_async_remote_copy(
        wo_ref.at[:, at_rows(there, width)],
        all_o.at[h, at_rows(me, wo_ref.shape[0]), :],
        os_,
        or_,
        peer,
        MESH,
    )
    half.start()
    net.own(0, start)

    def x_copy(j):
        source, target = x_part(j)
        return pltpu.make_async_remote_copy(source, target, xs.at[j], xr.at[j], peer, MESH)

    for j in range(4):
        x_copy(j).start()

    def out_own():
        mine[1].wait()
        half.wait_recv()
        net.own(1, start)

    def out_twin():
        net.twin(1, start)

    L = lambda t, s: lambda: net.line(t, s, start)
    A = lambda t, s: lambda: net.across(t, s, start)
    B = lambda t, s: lambda: net.both(t, s, start)
    S = lambda t: lambda: net.own(t, start, (SIDE,))
    U = lambda t: lambda: net.own(t, start, (UP, DOWN, CORE))
    before, during, after = sizes["plan"](L, A, B, S, U, out_own, out_twin)
    for n, step in enumerate(before):
        step()
        if n == 1:
            fill()
    net.rest(0)

    def project(j):
        at = at_rows(j, groups)
        n = norm_rows(x[at, :].astype(jnp.float32), par(g1, depth), par(b1, depth))

        def part(i):
            return jnp.dot(n, all_q[i], preferred_element_type=jnp.float32)

        q[at, :] = ((part(0) + par(qb, columns)) * HDIM ** (-0.5)).astype(jnp.bfloat16)
        k[at, :] = part(1).astype(jnp.bfloat16)
        v[at, :] = (part(2) + par(vb, columns)).astype(jnp.bfloat16)

    def x_wait(j):
        pltpu.make_async_copy(*x_part(j), xo.at[j]).wait()
        x_copy(j).wait_recv()

    def project_when_here(j):
        for n in range(4):
            pl.when(j == n)(lambda n=n: x_wait(n))
        project(j)

    loop(0, 4, project_when_here)

    lane = lax.broadcasted_iota(jnp.int32, (1, PAIR), 1)
    low_f = jnp.where(lane < HDIM, 1.0, 0.0)
    low, high = low_f.astype(jnp.bfloat16), (1.0 - low_f).astype(jnp.bfloat16)

    def attend(b, p):
        cols = at_rows(p, PAIR)
        keys, values = k[:, cols], v[:, cols]

        def head(query, value):
            scores = lax.dot_general(
                query, keys, (((1,), (1,)), ((), ())), preferred_element_type=jnp.float32
            )
            top = jnp.max(scores, axis=-1, keepdims=True)
            weights = jnp.exp(scores - top).astype(jnp.bfloat16)
            return jnp.dot(weights, value, preferred_element_type=jnp.float32)

        at = at_rows(b, block)
        query = q[at, cols]
        one = head(query * low, values * low + high)
        two = head(query * high, values * high + low)
        top = one * low_f + two * (1.0 - low_f)
        total = pltpu.roll(one * (1.0 - low_f) + two * low_f, HDIM, 1)
        ctx[at, at_rows(h * pairs + p, PAIR)] = (top / total).astype(jnp.bfloat16)

    def ctx_copy(b, p):
        ref = ctx.at[at_rows(b, block), at_rows(h * pairs + p, PAIR)]
        return pltpu.make_async_remote_copy(ref, ref, cs.at[b], cr.at[b], peer, MESH)

    def ctx_all(b):
        ref = ctx.at[at_rows(b, block), at_rows(h, columns)]
        return pltpu.make_async_remote_copy(ref, ref, cs.at[b], cr.at[b], peer, MESH)

    def attended(b):
        ctx_all(b).wait_recv()
        at = at_rows(b, block)
        total = x[at, at_rows(h, width)].astype(jnp.float32) + par(ob, width)
        for i in range(2):
            total = total + jnp.dot(
                ctx[at, i * columns : (i + 1) * columns],
                all_o[i],
                preferred_element_type=jnp.float32,
            )
        att[at, :] = total.astype(jnp.bfloat16)

    def piece(ref, b, j):
        return ref.at[at_rows(b * dp + j, rows)]

    def home(b, j):
        return full.at[at_rows(b * dp + j, rows), at_rows(h, width)]

    def one(b, n):
        other = lax.rem(me + n, dp)
        return pltpu.make_async_remote_copy(
            piece(att, b, other), home(b, me), s1.at[b], r1.at[b], (other, h), MESH
        )

    def one_all(b):
        ref = att.at[: (dp - 1) * rows]
        return pltpu.make_async_remote_copy(ref, ref, s1.at[b], r1.at[b], peer, MESH)

    def one_own(b):
        return pltpu.make_async_copy(piece(att, b, me), home(b, me), l1.at[b])

    def two(b, n):
        other = lax.rem(me + n, dp)
        return pltpu.make_async_remote_copy(
            second.at[b, other], piece(placed, b, me), s2.at[b], r2.at[b], (other, h), MESH
        )

    def two_all(b):
        ref = placed.at[: (dp - 1) * rows]
        return pltpu.make_async_remote_copy(ref, ref, s2.at[b], r2.at[b], peer, MESH)

    def two_own(b):
        return pltpu.make_async_copy(second.at[b, me], piece(placed, b, me), l2.at[b])

    def three(b):
        ref = full.at[at_rows(b, block), at_rows(h, width)]
        return pltpu.make_async_remote_copy(ref, ref, s3.at[b], r3.at[b], peer, MESH)

    def spread(b):
        one_own(b).start()
        loop(1, dp, lambda n: one(b, n).start())

    def arrive(b):
        one_own(b).wait()
        one_all(b).wait_recv()
        three(b).start()

    def share(b, target):
        return jnp.dot(
            hidden[at_rows(b, block), :],
            all_2[:, at_rows(target, width)],
            preferred_element_type=jnp.float32,
        )

    def out_copy(b):
        return pltpu.make_async_remote_copy(
            out.at[b], got.at[b], fs.at[b], fr.at[b], peer, MESH
        )

    def feed(b):
        three(b).wait_recv()
        at = at_rows(b, block)
        normed[...] = norm_rows(full[at, :].astype(jnp.float32), par(g2, depth), par(b2, depth))

        for t in range(units // tile):
            cols = slice(t * tile, (t + 1) * tile)
            sums = jnp.dot(normed[...], all_1[:, cols], preferred_element_type=jnp.float32)
            sums = sums + par(f1 + t * tile, tile)
            hidden[at, cols] = (0.5 * sums * (1.0 + lax.erf(sums * 0.7071067811865476))).astype(
                jnp.bfloat16
            )

        out[b] = share(b, there).astype(jnp.bfloat16)
        out_copy(b).start()

    def done_copy(b, i):
        n = b * (block // chunk) + i
        per = groups // chunk
        return pltpu.make_async_copy(
            placed.at[at_rows(n, chunk)],
            o_ref.at[at_rows(lax.rem(n, per), chunk), at_rows(lax.div(n, per), width)],
            ds.at[b, i],
        )

    def close(b):
        at = at_rows(b, block)
        kept = full[at, at_rows(h, width)].astype(jnp.float32) + par(fb, width) + share(b, h)
        out_copy(b).wait_recv()
        total = (kept + got[b].astype(jnp.float32)).astype(jnp.bfloat16)
        done[...] = total.reshape(dp, rows, width)

        def choose(s):
            second[b, s] = done[order_ref[s]]

        loop(0, dp, choose)
        two_own(b).start()
        loop(1, dp, lambda n: two(b, n).start())

    def store(b):
        two_own(b).wait()
        two_all(b).wait_recv()
        loop(0, block // chunk, lambda i: done_copy(b, i).start())

    def when(i, offset, body):
        b = i - offset

        @pl.when((b >= 0) & (b < blocks))
        def _():
            body(b)

    o_arrive, o_feed, o_close, o_store = sizes["stages"]

    def run(table, at):
        for n, steps in table.items():

            @pl.when(at == n)
            def _(steps=steps):
                for step in steps:
                    step()

    def sent():
        half.wait_send()
        for j in range(4):
            x_copy(j).wait_send()

        def block_sent(b):
            ctx_all(b).wait_send()
            one_all(b).wait_send()

        loop(0, blocks, block_sent)
        for t in range(5):
            net.finish(t, t == 1)

    def master(i):
        def out_block(b):
            pl.when(b == 0)(lambda: net.rest(1))
            attended(b)
            spread(b)

        def attend_block(b):
            def each(p):
                attend(b, p)
                ctx_copy(b, p).start()
                pl.when((p == 1) & (b > 0))(lambda: out_block(b - 1))
                run(during, b * pairs + p)

            loop(0, pairs, each)

        when(i, 0, attend_block)
        pl.when(i == blocks)(lambda: out_block(blocks - 1))
        run(after, i)
        when(i, o_arrive, arrive)

        def feed_block(b):
            @pl.when(b == 0)
            def _():
                for t in (2, 3, 4):
                    net.rest(t)

            feed(b)

        when(i, o_feed, feed_block)

        def close_block(b):
            pl.when(b == 0)(lambda: net.rest(5))
            close(b)
            pl.when(b == 0)(sent)
            pl.when(b == 1)(lambda: net.finish(5, False))

        when(i, o_close, close_block)
        when(i, o_store, store)

    loop(0, blocks + o_store, master)

    def last(b):
        three(b).wait_send()
        out_copy(b).wait_send()
        two_all(b).wait_send()
        loop(0, block // chunk, lambda i: done_copy(b, i).wait())

    loop(0, blocks, last)


def plan(L, A, B, S, U, out_own, out_twin):
    before = [
        out_own, S(2), L(0, 1), out_twin, B(1, 1), U(2), L(0, 2), S(3), A(0, 0), A(0, 1), B(1, 2),
        U(3), L(0, 3), S(4), U(4), A(0, 2), L(2, 1), A(0, 3),
    ]
    during = {
        0: [L(3, 1)], 1: [B(1, 3)], 2: [L(4, 1)], 6: [L(2, 2)], 10: [L(3, 2)], 13: [L(4, 2)],
        16: [L(2, 3)], 19: [L(3, 3)],
    }
    after = {
        4: [S(5), U(5)], 5: [L(4, 3), A(2, 0), A(3, 0), A(4, 0), A(2, 1), A(3, 1), A(4, 1)],
        6: [L(5, 1), A(2, 2), A(3, 2), A(4, 2), A(2, 3), A(3, 3)], 7: [L(5, 2), A(4, 3)],
        8: [L(5, 3), A(5, 0)], 9: [A(5, 1)], 10: [A(5, 2)], 11: [A(5, 3)],
    }
    return before, during, after


def on_device_aligned(
    frames_in,
    ln1_gain,
    ln1_bias,
    qkv_weight,
    qv_bias,
    out_weight,
    out_bias,
    ln2_gain,
    ln2_bias,
    fc1_weight,
    fc1_bias,
    fc2_weight,
    fc2_bias,
    server_of_clip,
):
    dp, heads = lax.axis_size("dp"), lax.axis_size("head")
    groups, width = frames_in.shape[2], frames_in.shape[3] // 4
    frames, depth = groups * 4, width * heads
    rows = 16
    blocks = frames // (dp * rows)
    block = dp * rows
    columns, units = qkv_weight.shape[2], fc1_weight.shape[1]
    values = [
        ln1_gain, ln1_bias, ln2_gain, ln2_bias, qv_bias, out_bias, fc2_bias, fc1_bias
    ]
    base = 4 * depth
    offsets = (
        (0, depth),
        (2 * depth, 3 * depth),
        base,
        base + columns,
        base + 2 * columns,
        base + 2 * columns + width,
        base + 2 * columns + 2 * width,
    )
    sizes = {
        "tile": 512,
        "chunk": 64,
        "offsets": offsets,
        "lengths": [value.shape[-1] for value in values],
        "plan": plan,
        "stages": (3, 7, 12, 14),
    }
    bf16, f32 = jnp.bfloat16, jnp.float32
    dma = pltpu.SemaphoreType.DMA
    out = pl.pallas_call(
        functools.partial(layer_kernel, dp, sizes),
        out_shape=jax.ShapeDtypeStruct((groups, 4 * width), bf16),
        in_specs=[
            pl.BlockSpec(memory_space=pltpu.MemorySpace.SMEM),
        ]
        + [pl.BlockSpec(memory_space=ANY)] * (5 + len(values)),
        out_specs=pl.BlockSpec(memory_space=ANY),
        scratch_shapes=[
            pltpu.VMEM((3, depth, columns), bf16),
            pltpu.VMEM((heads, columns, width), bf16),
            pltpu.VMEM((depth, units), bf16),
            pltpu.VMEM((units, depth), bf16),
            pltpu.VMEM((frames, depth), bf16),
            pltpu.VMEM((frames, columns), bf16),
            pltpu.VMEM((frames, columns), bf16),
            pltpu.VMEM((frames, columns), bf16),
            pltpu.VMEM((frames, heads * columns), bf16),
            pltpu.VMEM((frames, width), bf16),
            pltpu.VMEM((blocks, dp, rows, width), bf16),
            pltpu.VMEM((frames, depth), bf16),
            pltpu.VMEM((block, depth), bf16),
            pltpu.VMEM((frames, units), bf16),
            pltpu.VMEM((blocks, block, width), bf16),
            pltpu.VMEM((blocks, block, width), bf16),
            pltpu.VMEM((dp, rows, width), bf16),
            pltpu.VMEM((frames, width), bf16),
            dma((6, 4)),
            dma((6, dp // CORES)),
            dma((6,)),
            dma((4,)),
            dma((4,)),
            dma((4,)),
            dma((4,)),
            dma,
            dma,
            dma((blocks,)),
            dma((blocks,)),
            dma((blocks,)),
            dma((blocks,)),
            dma((blocks,)),
            dma((blocks,)),
            dma((blocks,)),
            dma((blocks,)),
            dma((blocks,)),
            dma((blocks,)),
            dma((blocks,)),
            dma((blocks,)),
            dma((blocks, block // sizes["chunk"])),
            pltpu.VMEM((1, sum(value.size for value in values)), f32),
            *[pltpu.VMEM(value.shape, f32) for value in values],
            dma((len(values),)),
        ],
        compiler_params=pltpu.CompilerParams(
            collective_id=0, has_side_effects=True, vmem_limit_bytes=66000000
        ),
        name="layer",
    )(
        slot_order(server_of_clip),
        *values,
        frames_in[0, 0],
        jnp.swapaxes(qkv_weight, 0, 1),
        out_weight,
        fc1_weight,
        fc2_weight,
    )
    return out[None, None]


def aligned(mesh, frames_in, qkv_weight, out_weight, fc1_weight):
    dp, heads = mesh.shape["dp"], mesh.shape["head"]
    groups, width = frames_in.shape[2], frames_in.shape[3] // 4
    frames = groups * 4
    return (
        dp % 4 == 0
        and dp >= 16
        and heads == 2
        and frames % (dp * 16) == 0
        and groups % 64 == 0
        and (dp * 16) % 64 == 0
        and width % 128 == 0
        and out_weight.shape[0] % (dp * heads * 16) == 0
        and (qkv_weight.shape[2] // heads) % PAIR == 0
        and (qkv_weight.shape[0] // dp) % 16 == 0
        and (fc1_weight.shape[1] // heads) % 512 == 0
    )


def solution(mesh):
    placed = (
        P("dp", "head", None, None),
        P(),
        P(),
        P("dp", None, "head"),
        P(None, "head"),
        P(("head", "dp"), None),
        P("head"),
        P(),
        P(),
        P("dp", "head"),
        P("head"),
        P(("head", "dp"), None),
        P("head"),
        P(),
    )

    def layer(*args):
        body = on_device_aligned if aligned(mesh, args[0], args[3], args[5], args[9]) else on_device
        return jax.shard_map(
            body,
            mesh=mesh,
            in_specs=placed,
            out_specs=P("dp", "head", None, None),
            check_vma=False,
        )(*args)

    return layer
```

```python
import functools

import jax
import jax.numpy as jnp
from jax import lax
from jax.experimental import pallas as pl
from jax.experimental.pallas import tpu as pltpu
from jax.sharding import PartitionSpec as P

HDIM = 64


epsilon = 1e-05


def layer_norm(matrix, gain_row, shift_row):
    floats = matrix.astype(jnp.float32)
    center = jnp.mean(floats, axis=-1, keepdims=True)
    spread = jnp.mean(jnp.square(floats - center), axis=-1, keepdims=True)
    return ((floats - center) * lax.rsqrt(spread + epsilon) * gain_row + shift_row).astype(
        jnp.bfloat16
    )


def normalize(residual_in, gain_row, shift_row):
    whole_rows = lax.all_gather(residual_in, "head", axis=1, tiled=True)
    return layer_norm(whole_rows, gain_row, shift_row)


def attend(queries, key_rows, value_rows):

    def single(triple):
        query_head, key_head, value_head = triple
        scores = jnp.dot(query_head, key_head.T, preferred_element_type=jnp.float32)
        maxima = jnp.max(scores, axis=-1, keepdims=True)
        weights = jnp.exp(scores - maxima)
        probability = (weights / jnp.sum(weights, axis=-1, keepdims=True)).astype(jnp.bfloat16)
        return jnp.dot(probability, value_head, preferred_element_type=jnp.float32).astype(
            jnp.bfloat16
        )

    per_head = lax.map(
        single,
        (jnp.swapaxes(queries, 0, 1), jnp.swapaxes(key_rows, 0, 1), jnp.swapaxes(value_rows, 0, 1)),
    )
    return jnp.swapaxes(per_head, 0, 1).reshape(queries.shape[0], -1)


def slot_order(server_list):
    clip_count = server_list.shape[0]
    indices = jnp.arange(clip_count, dtype=jnp.int32)
    earlier = (server_list[None, :] < server_list[:, None]) | (
        server_list[None, :] == server_list[:, None]
    ) & (indices[None, :] < indices[:, None])
    slot_of = jnp.sum(earlier.astype(jnp.int32), axis=1)
    return jnp.sum(jnp.where(slot_of[None, :] == indices[:, None], indices[None, :], 0), axis=1)


def regroup(block_rows, clip_order):
    group_size = lax.axis_size("dp")
    piece_rows = block_rows.reshape(group_size, -1)
    shuffled = lax.all_to_all(piece_rows, "dp", split_axis=0, concat_axis=0, tiled=True)
    picked = jnp.take(shuffled, clip_order, axis=0)
    returned = lax.all_to_all(picked, "dp", split_axis=0, concat_axis=0, tiled=True)
    return returned.reshape(block_rows.shape)


def block_term(operand, weight_rows, row_count, frame_count, local_width):
    blocks = row_count // frame_count
    product = jnp.dot(operand, weight_rows, preferred_element_type=jnp.float32)
    return (
        product.reshape(frame_count, blocks, local_width)
        .transpose(1, 0, 2)
        .reshape(blocks * frame_count, local_width)
    )


def on_device(
    frames_in,
    ln1_gain,
    ln1_bias,
    qkv_weight,
    qv_bias,
    out_weight,
    out_bias,
    ln2_gain,
    ln2_bias,
    fc1_weight,
    fc1_bias,
    fc2_weight,
    fc2_bias,
    server_of_clip,
):
    clip_order = slot_order(server_of_clip)
    group_rows = frames_in.shape[2]
    local_width = frames_in.shape[3] // 4
    frame_count = group_rows * 4
    residual_in = frames_in[0, 0].reshape(frame_count, local_width)
    residual_in = regroup(residual_in, clip_order)
    normed_one = normalize(residual_in, ln1_gain, ln1_bias)
    column_count = qkv_weight.shape[2]
    weight_piece = lax.all_gather(qkv_weight, "dp", axis=0, tiled=True)
    operand = normed_one
    projected = jnp.dot(
        operand, weight_piece.reshape(weight_piece.shape[0], -1), preferred_element_type=jnp.float32
    ).reshape(frame_count, 3, column_count)
    queries = (
        ((projected[:, 0] + qv_bias[0]) * HDIM ** (-0.5))
        .astype(jnp.bfloat16)
        .reshape(frame_count, -1, HDIM)
    )
    key_rows = projected[:, 1].astype(jnp.bfloat16).reshape(frame_count, -1, HDIM)
    value_rows = (projected[:, 2] + qv_bias[1]).astype(jnp.bfloat16).reshape(frame_count, -1, HDIM)
    context = attend(queries, key_rows, value_rows)
    output_rows = lax.all_gather(out_weight, "dp", axis=0, tiled=True)
    carried = residual_in.astype(jnp.float32) + out_bias
    attended = (
        carried
        + lax.psum_scatter(
            block_term(
                context, output_rows, frame_count * lax.axis_size("head"), frame_count, local_width
            ).astype(jnp.bfloat16),
            "head",
            scatter_dimension=0,
            tiled=True,
        ).astype(jnp.float32)
    ).astype(jnp.bfloat16)
    normed_two = normalize(attended, ln2_gain, ln2_bias)
    operand = normed_two
    hidden_sums = jnp.dot(
        operand,
        lax.all_gather(fc1_weight, "dp", axis=0, tiled=True),
        preferred_element_type=jnp.float32,
    )
    hidden = jax.nn.gelu(hidden_sums + fc1_bias, approximate=False).astype(jnp.bfloat16)
    down_rows = lax.all_gather(fc2_weight, "dp", axis=0, tiled=True)
    kept = attended.astype(jnp.float32) + fc2_bias
    layer_out = (
        kept
        + lax.psum_scatter(
            block_term(
                hidden, down_rows, frame_count * lax.axis_size("head"), frame_count, local_width
            ).astype(jnp.bfloat16),
            "head",
            scatter_dimension=0,
            tiled=True,
        ).astype(jnp.float32)
    ).astype(jnp.bfloat16)
    return layer_out.reshape(1, 1, group_rows, 4 * local_width)


MESH = pl.DeviceIdType.MESH
VMEM = pltpu.MemorySpace.VMEM
ANY = pl.ANY
CORES = 2
PAIR = 2 * HDIM
UP, DOWN, SIDE, CORE = range(4)


def at_rows(index, rows):
    return pl.ds(pl.multiple_of(index * rows, rows), rows)


def norm_rows(floats, gain, shift):
    center = jnp.mean(floats, axis=-1, keepdims=True)
    moved = floats - center
    spread = jnp.mean(jnp.square(moved), axis=-1, keepdims=True)
    return (moved * lax.rsqrt(spread + epsilon) * gain + shift).astype(jnp.bfloat16)


def loop(start, stop, body):
    def step(k, carry):
        body(k)
        return carry

    lax.fori_loop(start, stop, step, 0)


class Gather:
    def __init__(self, me, h, dp, parts, send, recv, near):
        self.h, self.parts, self.send, self.recv, self.near = h, parts, send, recv, near
        self.sides = 2
        self.length = dp // (self.sides * CORES)
        self.core = lax.rem(me, CORES)
        self.side = lax.rem(lax.div(me, CORES), self.sides)
        self.z = lax.div(me, CORES * self.sides)

    def index(self, z, side, core):
        return (z * self.sides + side) * CORES + core

    def copy(self, t, origin, route, count=1):
        target = {
            UP: lambda: self.index(self.z + 1, self.side, self.core),
            DOWN: lambda: self.index(self.z - 1, self.side, self.core),
            SIDE: lambda: self.index(self.z, 1 - self.side, self.core),
            CORE: lambda: self.index(self.z, self.side, 1 - self.core),
        }[route]()
        ref = self.parts[t](origin, count)
        near = self.near.at[t] if route == CORE else self.recv.at[t, lax.div(origin, CORES)]
        return pltpu.make_async_remote_copy(
            ref, ref, self.send.at[t, route], near, (target, self.h), MESH
        )

    def go(self, t, origin, routes, act):
        for route in routes:
            copy = self.copy(t, origin, route)
            if route == UP:
                pl.when(self.z < self.length - 1)(lambda copy=copy: act(copy))
            elif route == DOWN:
                pl.when(self.z > 0)(lambda copy=copy: act(copy))
            else:
                act(copy)

    def own(self, t, act, routes=(UP, DOWN, SIDE, CORE)):
        self.go(t, self.index(self.z, self.side, self.core), routes, act)

    def line(self, t, s, act):
        @pl.when(self.z >= s)
        def _():
            origin = self.index(self.z - s, self.side, self.core)
            self.copy(t, origin, SIDE).wait_recv()
            self.go(t, origin, (UP, SIDE, CORE), act)

        @pl.when(self.z + s < self.length)
        def _():
            origin = self.index(self.z + s, self.side, self.core)
            self.copy(t, origin, SIDE).wait_recv()
            self.go(t, origin, (DOWN, SIDE, CORE), act)

    def across(self, t, s, act):
        def one(z):
            origin = self.index(z, 1 - self.side, self.core)
            self.copy(t, origin, SIDE).wait_recv()
            self.go(t, origin, (CORE,), act)

        if s == 0:
            one(self.z)
            return
        pl.when(self.z >= s)(lambda: one(self.z - s))
        pl.when(self.z + s < self.length)(lambda: one(self.z + s))

    def twin(self, t, act):
        origin = self.index(self.z, 1 - self.side, self.core)
        self.copy(t, origin, SIDE).wait_recv()
        self.go(t, origin, (UP, DOWN, CORE), act)

    def both(self, t, s, act):
        def one(z, route):
            for side in range(self.sides):
                origin = self.index(z, side, self.core)
                self.copy(t, origin, SIDE).wait_recv()
                self.go(t, origin, (route, CORE), act)

        pl.when(self.z >= s)(lambda: one(self.z - s, UP))
        pl.when(self.z + s < self.length)(lambda: one(self.z + s, DOWN))

    def rest(self, t):
        self.copy(t, 0, CORE, self.length * self.sides).wait_recv()

    def finish(self, t, paired):
        each = self.sides if paired else 1
        self.copy(t, 0, CORE, self.length * self.sides).wait_send()
        self.copy(t, 0, SIDE, 1 if paired else self.length).wait_send()
        for z in range(self.length - 1):
            up = self.copy(t, 0, UP, (z + 1) * each)
            pl.when(self.z == z)(lambda copy=up: copy.wait_send())
            down = self.copy(t, 0, DOWN, (z + 1) * each)
            pl.when(self.z == self.length - 1 - z)(lambda copy=down: copy.wait_send())


def layer_kernel(
    dp,
    sizes,
    order_ref,
    *refs,
):
    count = len(sizes["lengths"])
    values, refs = refs[:count], refs[count:]
    par_ref, par_sem, flat, refs = refs[-2 - count], refs[-1], refs[-1 - count : -1], refs[: -2 - count]
    copies = [
        pltpu.make_async_copy(value, part, par_sem.at[n])
        for n, (value, part) in enumerate(zip(values, flat))
    ]
    for copy in copies:
        copy.start()

    def fill():
        offset = 0
        for copy, part, length in zip(copies, flat, sizes["lengths"]):
            copy.wait()
            for row in range(part.shape[0] if len(part.shape) == 2 else 1):
                line = part[row : row + 1, :] if len(part.shape) == 2 else part[...][None, :]
                par_ref[0:1, offset : offset + length] = line
                offset += length

    layer_body(dp, sizes, order_ref, par_ref, fill, *refs)


def layer_body(
    dp,
    sizes,
    order_ref,
    par_ref,
    fill,
    x_ref,
    wq_ref,
    wo_ref,
    w1_ref,
    w2_ref,
    o_ref,
    all_q,
    all_o,
    all_1,
    all_2,
    x,
    q,
    k,
    v,
    ctx,
    att,
    second,
    full,
    normed,
    hidden,
    out,
    got,
    done,
    placed,
    wsend,
    wrecv,
    wnear,
    own_sem,
    xs,
    xr,
    xo,
    os_,
    or_,
    cs,
    cr,
    s1,
    r1,
    l1,
    s2,
    r2,
    l2,
    s3,
    r3,
    fs,
    fr,
    ds,
):
    start = lambda copy: copy.start()
    me, h = lax.axis_index("dp"), lax.axis_index("head")
    there = 1 - h
    peer = (me, there)
    groups = x_ref.shape[0]
    width = x_ref.shape[1] // 4
    frames, depth = x.shape
    columns, units = q.shape[1], w1_ref.shape[1]
    pairs = columns // PAIR
    blocks, _, rows, _ = second.shape
    block = frames // blocks
    tile = sizes["tile"]
    chunk = sizes["chunk"]
    (g1, b1), (g2, b2), qb, vb, ob, fb, f1 = sizes["offsets"]

    def par(offset, size):
        return par_ref[0:1, offset : offset + size]

    barrier = pltpu.get_barrier_semaphore()

    def hello(n):
        pl.semaphore_signal(barrier, inc=1, device_id=(lax.rem(me + n, dp), h), device_id_type=MESH)

    loop(1, dp, hello)
    pl.semaphore_signal(barrier, inc=1, device_id=peer, device_id_type=MESH)

    def span(d, rows, count):
        return pl.ds(pl.multiple_of(d * rows, rows), rows * count)

    parts = [
        lambda d, n=1: all_q.at[:, span(d, wq_ref.shape[1], n), :],
        lambda d, n=1: all_o.at[:, span(d, wo_ref.shape[0], n), :],
        lambda d, n=1: all_1.at[span(d, w1_ref.shape[0], n), : units // 2],
        lambda d, n=1: all_1.at[span(d, w1_ref.shape[0], n), units // 2 :],
        lambda d, n=1: all_2.at[span(d, w2_ref.shape[0], n), at_rows(there, width)],
        lambda d, n=1: all_2.at[span(d, w2_ref.shape[0], n), at_rows(h, width)],
    ]
    net = Gather(me, h, dp, parts, wsend, wrecv, wnear)
    mine = [
        pltpu.make_async_copy(wq_ref, parts[0](me), own_sem.at[0]),
        pltpu.make_async_copy(
            wo_ref.at[:, at_rows(h, width)],
            all_o.at[h, at_rows(me, wo_ref.shape[0]), :],
            own_sem.at[1],
        ),
        pltpu.make_async_copy(w1_ref, all_1.at[at_rows(me, w1_ref.shape[0]), :], own_sem.at[2]),
        pltpu.make_async_copy(w2_ref, all_2.at[at_rows(me, w2_ref.shape[0]), :], own_sem.at[3]),
    ]
    for copy in mine:
        copy.start()

    def x_part(j):
        return x_ref.at[:, j * width : (j + 1) * width], x.at[
            j * groups : (j + 1) * groups, at_rows(h, width)
        ]

    for j in range(4):
        pltpu.make_async_copy(*x_part(j), xo.at[j]).start()
    for n in (0, 2, 3):
        mine[n].wait()
    pl.semaphore_wait(barrier, dp)

    half = pltpu.make_async_remote_copy(
        wo_ref.at[:, at_rows(there, width)],
        all_o.at[h, at_rows(me, wo_ref.shape[0]), :],
        os_,
        or_,
        peer,
        MESH,
    )
    half.start()
    net.own(0, start)

    def x_copy(j):
        source, target = x_part(j)
        return pltpu.make_async_remote_copy(source, target, xs.at[j], xr.at[j], peer, MESH)

    for j in range(4):
        x_copy(j).start()

    def out_own():
        mine[1].wait()
        half.wait_recv()
        net.own(1, start)

    def out_twin():
        net.twin(1, start)

    L = lambda t, s: lambda: net.line(t, s, start)
    A = lambda t, s: lambda: net.across(t, s, start)
    B = lambda t, s: lambda: net.both(t, s, start)
    S = lambda t: lambda: net.own(t, start, (SIDE,))
    U = lambda t: lambda: net.own(t, start, (UP, DOWN, CORE))
    before, during, after = sizes["plan"](L, A, B, S, U, out_own, out_twin)
    for n, step in enumerate(before):
        step()
        if n == 1:
            fill()
    net.rest(0)

    def project(j):
        at = at_rows(j, groups)
        n = norm_rows(x[at, :].astype(jnp.float32), par(g1, depth), par(b1, depth))

        def part(i):
            return jnp.dot(n, all_q[i], preferred_element_type=jnp.float32)

        q[at, :] = ((part(0) + par(qb, columns)) * HDIM ** (-0.5)).astype(jnp.bfloat16)
        k[at, :] = part(1).astype(jnp.bfloat16)
        v[at, :] = (part(2) + par(vb, columns)).astype(jnp.bfloat16)

    def x_wait(j):
        pltpu.make_async_copy(*x_part(j), xo.at[j]).wait()
        x_copy(j).wait_recv()

    def project_when_here(j):
        for n in range(4):
            pl.when(j == n)(lambda n=n: x_wait(n))
        project(j)

    loop(0, 4, project_when_here)

    lane = lax.broadcasted_iota(jnp.int32, (1, PAIR), 1)
    low_f = jnp.where(lane < HDIM, 1.0, 0.0)
    low, high = low_f.astype(jnp.bfloat16), (1.0 - low_f).astype(jnp.bfloat16)

    def attend(b, p):
        cols = at_rows(p, PAIR)
        keys, values = k[:, cols], v[:, cols]

        def head(query, value):
            scores = lax.dot_general(
                query, keys, (((1,), (1,)), ((), ())), preferred_element_type=jnp.float32
            )
            top = jnp.max(scores, axis=-1, keepdims=True)
            weights = jnp.exp(scores - top).astype(jnp.bfloat16)
            return jnp.dot(weights, value, preferred_element_type=jnp.float32)

        at = at_rows(b, block)
        query = q[at, cols]
        one = head(query * low, values * low + high)
        two = head(query * high, values * high + low)
        top = one * low_f + two * (1.0 - low_f)
        total = pltpu.roll(one * (1.0 - low_f) + two * low_f, HDIM, 1)
        ctx[at, at_rows(h * pairs + p, PAIR)] = (top / total).astype(jnp.bfloat16)

    def ctx_copy(b, p):
        ref = ctx.at[at_rows(b, block), at_rows(h * pairs + p, PAIR)]
        return pltpu.make_async_remote_copy(ref, ref, cs.at[b], cr.at[b], peer, MESH)

    def ctx_all(b):
        ref = ctx.at[at_rows(b, block), at_rows(h, columns)]
        return pltpu.make_async_remote_copy(ref, ref, cs.at[b], cr.at[b], peer, MESH)

    def attended(b):
        ctx_all(b).wait_recv()
        at = at_rows(b, block)
        total = x[at, at_rows(h, width)].astype(jnp.float32) + par(ob, width)
        for i in range(2):
            total = total + jnp.dot(
                ctx[at, i * columns : (i + 1) * columns],
                all_o[i],
                preferred_element_type=jnp.float32,
            )
        att[at, :] = total.astype(jnp.bfloat16)

    def piece(ref, b, j):
        return ref.at[at_rows(b * dp + j, rows)]

    def home(b, j):
        return full.at[at_rows(b * dp + j, rows), at_rows(h, width)]

    def one(b, n):
        other = lax.rem(me + n, dp)
        return pltpu.make_async_remote_copy(
            piece(att, b, other), home(b, me), s1.at[b], r1.at[b], (other, h), MESH
        )

    def one_all(b):
        ref = att.at[: (dp - 1) * rows]
        return pltpu.make_async_remote_copy(ref, ref, s1.at[b], r1.at[b], peer, MESH)

    def one_own(b):
        return pltpu.make_async_copy(piece(att, b, me), home(b, me), l1.at[b])

    def two(b, n):
        other = lax.rem(me + n, dp)
        return pltpu.make_async_remote_copy(
            second.at[b, other], piece(placed, b, me), s2.at[b], r2.at[b], (other, h), MESH
        )

    def two_all(b):
        ref = placed.at[: (dp - 1) * rows]
        return pltpu.make_async_remote_copy(ref, ref, s2.at[b], r2.at[b], peer, MESH)

    def two_own(b):
        return pltpu.make_async_copy(second.at[b, me], piece(placed, b, me), l2.at[b])

    def three(b):
        ref = full.at[at_rows(b, block), at_rows(h, width)]
        return pltpu.make_async_remote_copy(ref, ref, s3.at[b], r3.at[b], peer, MESH)

    def spread(b):
        one_own(b).start()
        loop(1, dp, lambda n: one(b, n).start())

    def arrive(b):
        one_own(b).wait()
        one_all(b).wait_recv()
        three(b).start()

    def share(b, target):
        return jnp.dot(
            hidden[at_rows(b, block), :],
            all_2[:, at_rows(target, width)],
            preferred_element_type=jnp.float32,
        )

    def out_copy(b):
        return pltpu.make_async_remote_copy(
            out.at[b], got.at[b], fs.at[b], fr.at[b], peer, MESH
        )

    def feed(b):
        three(b).wait_recv()
        at = at_rows(b, block)
        normed[...] = norm_rows(full[at, :].astype(jnp.float32), par(g2, depth), par(b2, depth))

        for t in range(units // tile):
            cols = slice(t * tile, (t + 1) * tile)
            sums = jnp.dot(normed[...], all_1[:, cols], preferred_element_type=jnp.float32)
            sums = sums + par(f1 + t * tile, tile)
            hidden[at, cols] = (0.5 * sums * (1.0 + lax.erf(sums * 0.7071067811865476))).astype(
                jnp.bfloat16
            )

        out[b] = share(b, there).astype(jnp.bfloat16)
        out_copy(b).start()

    def done_copy(b, i):
        n = b * (block // chunk) + i
        per = groups // chunk
        return pltpu.make_async_copy(
            placed.at[at_rows(n, chunk)],
            o_ref.at[at_rows(lax.rem(n, per), chunk), at_rows(lax.div(n, per), width)],
            ds.at[b, i],
        )

    def close(b):
        at = at_rows(b, block)
        kept = full[at, at_rows(h, width)].astype(jnp.float32) + par(fb, width) + share(b, h)
        out_copy(b).wait_recv()
        total = (kept + got[b].astype(jnp.float32)).astype(jnp.bfloat16)
        done[...] = total.reshape(dp, rows, width)

        def choose(s):
            second[b, s] = done[order_ref[s]]

        loop(0, dp, choose)
        two_own(b).start()
        loop(1, dp, lambda n: two(b, n).start())

    def store(b):
        two_own(b).wait()
        two_all(b).wait_recv()
        loop(0, block // chunk, lambda i: done_copy(b, i).start())

    def when(i, offset, body):
        b = i - offset

        @pl.when((b >= 0) & (b < blocks))
        def _():
            body(b)

    o_arrive, o_feed, o_close, o_store = sizes["stages"]

    def run(table, at):
        for n, steps in table.items():

            @pl.when(at == n)
            def _(steps=steps):
                for step in steps:
                    step()

    def sent():
        half.wait_send()
        for j in range(4):
            x_copy(j).wait_send()

        def block_sent(b):
            ctx_all(b).wait_send()
            one_all(b).wait_send()

        loop(0, blocks, block_sent)
        for t in range(5):
            net.finish(t, t == 1)

    def master(i):
        def out_block(b):
            pl.when(b == 0)(lambda: net.rest(1))
            attended(b)
            spread(b)

        def attend_block(b):
            def each(p):
                attend(b, p)
                ctx_copy(b, p).start()
                pl.when((p == 1) & (b > 0))(lambda: out_block(b - 1))
                run(during, b * pairs + p)

            loop(0, pairs, each)

        when(i, 0, attend_block)
        pl.when(i == blocks)(lambda: out_block(blocks - 1))
        run(after, i)
        when(i, o_arrive, arrive)

        def feed_block(b):
            @pl.when(b == 0)
            def _():
                for t in (2, 3, 4):
                    net.rest(t)

            feed(b)

        when(i, o_feed, feed_block)

        def close_block(b):
            pl.when(b == 0)(lambda: net.rest(5))
            close(b)
            pl.when(b == 0)(sent)
            pl.when(b == 1)(lambda: net.finish(5, False))

        when(i, o_close, close_block)
        when(i, o_store, store)

    loop(0, blocks + o_store, master)

    def last(b):
        three(b).wait_send()
        out_copy(b).wait_send()
        two_all(b).wait_send()
        loop(0, block // chunk, lambda i: done_copy(b, i).wait())

    loop(0, blocks, last)


def plan(L, A, B, S, U, out_own, out_twin):
    before = [
        out_own, S(2), L(0, 1), out_twin, B(1, 1), U(2), L(0, 2), S(3), A(0, 0), A(0, 1), B(1, 2),
        L(0, 3), U(3), S(4), U(4), A(0, 2), L(2, 1), A(0, 3),
    ]
    during = {
        0: [L(3, 1)], 1: [B(1, 3)], 2: [L(4, 1)], 6: [L(2, 2)], 10: [L(3, 2)], 13: [L(4, 2)],
        16: [L(2, 3)], 19: [L(3, 3)],
    }
    after = {
        4: [S(5), U(5)], 5: [L(4, 3), A(2, 0), A(3, 0), A(4, 0), A(2, 1), A(3, 1), A(4, 1)],
        6: [L(5, 1), A(2, 2), A(3, 2), A(4, 2), A(2, 3), A(3, 3)], 7: [L(5, 2), A(4, 3)],
        8: [L(5, 3), A(5, 0)], 9: [A(5, 1)], 10: [A(5, 2)], 11: [A(5, 3)],
    }
    return before, during, after


def on_device_aligned(
    frames_in,
    ln1_gain,
    ln1_bias,
    qkv_weight,
    qv_bias,
    out_weight,
    out_bias,
    ln2_gain,
    ln2_bias,
    fc1_weight,
    fc1_bias,
    fc2_weight,
    fc2_bias,
    server_of_clip,
):
    dp, heads = lax.axis_size("dp"), lax.axis_size("head")
    groups, width = frames_in.shape[2], frames_in.shape[3] // 4
    frames, depth = groups * 4, width * heads
    rows = 16
    blocks = frames // (dp * rows)
    block = dp * rows
    columns, units = qkv_weight.shape[2], fc1_weight.shape[1]
    values = [
        ln1_gain, ln1_bias, ln2_gain, ln2_bias, qv_bias, out_bias, fc2_bias, fc1_bias
    ]
    base = 4 * depth
    offsets = (
        (0, depth),
        (2 * depth, 3 * depth),
        base,
        base + columns,
        base + 2 * columns,
        base + 2 * columns + width,
        base + 2 * columns + 2 * width,
    )
    sizes = {
        "tile": 512,
        "chunk": 64,
        "offsets": offsets,
        "lengths": [value.shape[-1] for value in values],
        "plan": plan,
        "stages": (3, 7, 12, 14),
    }
    bf16, f32 = jnp.bfloat16, jnp.float32
    dma = pltpu.SemaphoreType.DMA
    out = pl.pallas_call(
        functools.partial(layer_kernel, dp, sizes),
        out_shape=jax.ShapeDtypeStruct((groups, 4 * width), bf16),
        in_specs=[
            pl.BlockSpec(memory_space=pltpu.MemorySpace.SMEM),
        ]
        + [pl.BlockSpec(memory_space=ANY)] * (5 + len(values)),
        out_specs=pl.BlockSpec(memory_space=ANY),
        scratch_shapes=[
            pltpu.VMEM((3, depth, columns), bf16),
            pltpu.VMEM((heads, columns, width), bf16),
            pltpu.VMEM((depth, units), bf16),
            pltpu.VMEM((units, depth), bf16),
            pltpu.VMEM((frames, depth), bf16),
            pltpu.VMEM((frames, columns), bf16),
            pltpu.VMEM((frames, columns), bf16),
            pltpu.VMEM((frames, columns), bf16),
            pltpu.VMEM((frames, heads * columns), bf16),
            pltpu.VMEM((frames, width), bf16),
            pltpu.VMEM((blocks, dp, rows, width), bf16),
            pltpu.VMEM((frames, depth), bf16),
            pltpu.VMEM((block, depth), bf16),
            pltpu.VMEM((frames, units), bf16),
            pltpu.VMEM((blocks, block, width), bf16),
            pltpu.VMEM((blocks, block, width), bf16),
            pltpu.VMEM((dp, rows, width), bf16),
            pltpu.VMEM((frames, width), bf16),
            dma((6, 4)),
            dma((6, dp // CORES)),
            dma((6,)),
            dma((4,)),
            dma((4,)),
            dma((4,)),
            dma((4,)),
            dma,
            dma,
            dma((blocks,)),
            dma((blocks,)),
            dma((blocks,)),
            dma((blocks,)),
            dma((blocks,)),
            dma((blocks,)),
            dma((blocks,)),
            dma((blocks,)),
            dma((blocks,)),
            dma((blocks,)),
            dma((blocks,)),
            dma((blocks,)),
            dma((blocks, block // sizes["chunk"])),
            pltpu.VMEM((1, sum(value.size for value in values)), f32),
            *[pltpu.VMEM(value.shape, f32) for value in values],
            dma((len(values),)),
        ],
        compiler_params=pltpu.CompilerParams(
            collective_id=0, has_side_effects=True, vmem_limit_bytes=66000000
        ),
        name="layer",
    )(
        slot_order(server_of_clip),
        *values,
        frames_in[0, 0],
        jnp.swapaxes(qkv_weight, 0, 1),
        out_weight,
        fc1_weight,
        fc2_weight,
    )
    return out[None, None]


def aligned(mesh, frames_in, qkv_weight, out_weight, fc1_weight):
    dp, heads = mesh.shape["dp"], mesh.shape["head"]
    groups, width = frames_in.shape[2], frames_in.shape[3] // 4
    frames = groups * 4
    return (
        dp % 4 == 0
        and dp >= 16
        and heads == 2
        and frames % (dp * 16) == 0
        and groups % 64 == 0
        and (dp * 16) % 64 == 0
        and width % 128 == 0
        and out_weight.shape[0] % (dp * heads * 16) == 0
        and (qkv_weight.shape[2] // heads) % PAIR == 0
        and (qkv_weight.shape[0] // dp) % 16 == 0
        and (fc1_weight.shape[1] // heads) % 512 == 0
    )


def solution(mesh):
    placed = (
        P("dp", "head", None, None),
        P(),
        P(),
        P("dp", None, "head"),
        P(None, "head"),
        P(("head", "dp"), None),
        P("head"),
        P(),
        P(),
        P("dp", "head"),
        P("head"),
        P(("head", "dp"), None),
        P("head"),
        P(),
    )

    def layer(*args):
        body = on_device_aligned if aligned(mesh, args[0], args[3], args[5], args[9]) else on_device
        return jax.shard_map(
            body,
            mesh=mesh,
            in_specs=placed,
            out_specs=P("dp", "head", None, None),
            check_vma=False,
        )(*args)

    return layer
```
